256 devices in a mesh: dp: 8 (over y, core), vocab: 32 (over x, z).
Axes of the slice: x: 4, y: 4, z: 8, core: 2. Of those that a mesh axis runs over, the one named last changes fastest.
Arguments:
- teacher_hidden: bfloat16 [1024, 16384], P('dp', 'vocab'), may hold values from -120 to 120
- student_hidden: bfloat16 [1024, 4096], P('dp', 'vocab'), may hold values from -120 to 120
- teacher_weight: bfloat16 [16384, 65536], P('dp', 'vocab'), may hold values from -1 to 1
- student_weight: bfloat16 [4096, 65536], P('dp', 'vocab'), may hold values from -1 to 1
Outputs:
- kl: float32 [1024], P('dp')
- loss: float32 [], replicated
The draws below stay inside these ranges and needn't reach their ends.
All inputs are finite; a program needn't handle non-finite values.
Results may differ from the reference program's by a relative error of at most 0.0003.
Values may be sent and summed in bfloat16 or wider, within the bound.
A program may use at most 128 MiB of HBM per device.

```python
import jax
import jax.numpy as jnp

HT = 16384
HS = 4096
V = 65536
TOKENS = 1024


def weight_block(key, offset, features, block_id):
    normals = jax.random.normal(jax.random.fold_in(jax.random.fold_in(key, offset), block_id), (features, 128), jnp.float32)
    return jnp.clip(normals, -6.0, 6.0) * features ** (-0.5)


def teacher_block(key, block_id):
    return weight_block(key, 101, HT, block_id)


def student_block(key, block_id):
    folded = teacher_block(key, block_id).reshape(HT // HS, HS, 128).sum(axis=0)
    own_noise = weight_block(key, 202, HS, block_id)
    return jnp.clip(folded + 0.1 * own_noise, -1.0, 1.0)


def stack_blocks(key, block_fn, features):
    tile_stack = jax.vmap(lambda block_id: block_fn(key, block_id))(jnp.arange(V // 128))
    return jnp.transpose(tile_stack, (1, 0, 2)).reshape(features, V)


def shared_rows(key):
    common = jax.random.normal(jax.random.fold_in(key, 11), (TOKENS, HS), jnp.float32) * 3.0
    rising = 1.0 + 0.85 * jnp.arange(TOKENS, dtype=jnp.float32) / TOKENS
    return (common, rising)


def draw_teacher_weight(key, part):
    return stack_blocks(key, teacher_block, HT).astype(jnp.bfloat16)


def draw_student_weight(key, part):
    return stack_blocks(key, student_block, HS).astype(jnp.bfloat16)


def draw_teacher_hidden(key, part):
    common, rising = shared_rows(key)
    own_noise = jax.random.normal(jax.random.fold_in(key, 12), (TOKENS, HT), jnp.float32) * 0.5 * rising[:, None]
    values = jnp.tile(common, (1, HT // HS)) + own_noise
    return jnp.clip(values, -120.0, 120.0).astype(jnp.bfloat16)


def draw_student_hidden(key, part):
    common, rising = shared_rows(key)
    own_noise = jax.random.normal(jax.random.fold_in(key, 32), (TOKENS, HS), jnp.float32) * 0.5 * rising[:, None]
    values = common + own_noise
    return jnp.clip(values, -120.0, 120.0).astype(jnp.bfloat16)


def setup_inputs(seed: int = 0) -> dict:
    keys = jax.random.split(jax.random.key(seed), 5)
    teacher_hidden = draw_teacher_hidden(jax.random.fold_in(keys[4], 71), 0)
    student_hidden = draw_student_hidden(jax.random.fold_in(keys[4], 71), 0)
    teacher_weight = draw_teacher_weight(jax.random.fold_in(keys[4], 71), 0)
    student_weight = draw_student_weight(jax.random.fold_in(keys[4], 71), 0)
    return dict(teacher_hidden=teacher_hidden, student_hidden=student_hidden, teacher_weight=teacher_weight, student_weight=student_weight)


def reference(teacher_hidden, student_hidden, teacher_weight, student_weight):
    teacher_logits = jnp.dot(teacher_hidden, teacher_weight, preferred_element_type=jnp.float32)
    student_logits = jnp.dot(student_hidden, student_weight, preferred_element_type=jnp.float32)
    teacher_top = jnp.max(teacher_logits, axis=1)
    student_top = jnp.max(student_logits, axis=1)
    teacher_exp = jnp.exp(teacher_logits - teacher_top[:, None])
    teacher_total = jnp.sum(teacher_exp, axis=1)
    weighted = jnp.sum(teacher_exp * (teacher_logits - student_logits), axis=1)
    student_total = jnp.sum(jnp.exp(student_logits - student_top[:, None]), axis=1)
    teacher_lse = teacher_top + jnp.log(teacher_total)
    student_lse = student_top + jnp.log(student_total)
    kl = weighted / teacher_total - teacher_lse + student_lse
    loss = jnp.mean(kl)
    return (kl, loss)
```

```python
import jax
import jax.numpy as jnp
from jax import lax
from jax.experimental import pallas as pl
from jax.experimental.pallas import tpu as pltpu
from jax.sharding import PartitionSpec as P

NX, NY, NZ = 4, 4, 8
TOK = 128
TF = 512
SF = 128
VB = 2048
CB = VB // NY
F32 = jnp.float32

OFFS = (0, -1, 1, -2, 2, -3, 3, 4)
STAGES = ((0, 128), (128, 256), (384, 128))
N_REMOTE = 100


def body(
    th, sh, tw, sw,
    kl_ref, loss_ref,
    tbuf, sbuf, twb, swb, swst, pbuf, ropp, rfin, slog, stat, st1, st2, st3, st4,
    ssem, rsem, lsem,
):
    dp = lax.axis_index("dp")
    v = lax.axis_index("vocab")
    y, c = lax.div(dp, 2), lax.rem(dp, 2)
    x, z = lax.div(v, NZ), lax.rem(v, NZ)
    o = 1 - c

    def dev(xx, yy, zz, cc):
        return (yy * 2 + cc, xx * NZ + zz)

    def xm(d):
        return lax.rem(x + (d + NX), NX)

    def ym(d):
        return lax.rem(y + (d + NY), NY)

    def zm(d):
        return lax.rem(z + (d + NZ), NZ)

    started = []
    count = [0]

    def copy_to(src, dst, device):
        i = count[0]
        count[0] += 1
        return pltpu.make_async_remote_copy(
            src_ref=src,
            dst_ref=dst,
            send_sem=ssem.at[i],
            recv_sem=rsem.at[i],
            device_id=device,
            device_id_type=pl.DeviceIdType.MESH,
        )

    def send(src, dst, device):
        d = copy_to(src, dst, device)
        d.start()
        started.append(d)
        return d

    tw_own = pltpu.make_async_copy(tw, twb.at[pl.ds(c * VB, VB), :], lsem.at[0])
    tw_own.start()
    sw_own = pltpu.make_async_copy(
        sw.at[:, :, pl.ds(y * CB, CB)], swb.at[pl.ds(c * 4, 4), pl.ds(y * SF, SF), :], lsem.at[1]
    )
    sw_own.start()
    sh_own = pltpu.make_async_copy(
        sh, sbuf.at[z, pl.ds(y * TOK, TOK), pl.ds(x * SF, SF)], lsem.at[2]
    )
    sh_own.start()

    def tshard(slot, zz, lo=0, n=TOK):
        return tbuf.at[pl.ds(slot * TOK + lo, n), pl.ds(zz * TF, TF)]

    th_own = pltpu.make_async_copy(th, tshard(0, z), lsem.at[3])

    @pl.when(x == y)
    def _():
        th_own.start()

    barrier = pltpu.get_barrier_semaphore()
    peers = [dev(xm(d), y, z, c) for d in range(1, NX)]
    peers += [dev(x, y, zm(d), c) for d in range(1, NZ)]
    peers += [(lax.rem(dp + d, 8), v) for d in range(1, 8)]
    for p in peers:
        pl.semaphore_signal(barrier, inc=1, device_id=p, device_id_type=pl.DeviceIdType.MESH)

    @pl.when(x != y)
    def _():
        pl.semaphore_signal(
            barrier, inc=1, device_id=dev(y, x, z, c), device_id_type=pl.DeviceIdType.MESH
        )
        pl.semaphore_wait(barrier, len(peers) + 1)

    @pl.when(x == y)
    def _():
        pl.semaphore_wait(barrier, len(peers))

    R, L = dev(xm(1), y, z, c), dev(xm(-1), y, z, c)
    U, D = dev(x, ym(1), z, c), dev(x, ym(-1), z, c)
    F, B = dev(x, y, zm(1), c), dev(x, y, zm(-1), c)
    mate = dev(x, y, z, o)

    th_move = copy_to(th, tshard(0, z), dev(y, x, z, c))

    @pl.when(x != y)
    def _():
        th_move.start()

    s_y = [
        send(
            sh,
            sbuf.at[z, pl.ds(y * TOK, TOK), pl.ds(x * SF, SF)],
            dev(x, ym(d), z, c),
        )
        for d in (1, -1, 2)
    ]

    opp = ym(2)
    sw_st_d = send(sw.at[pl.ds(0, 2), :, pl.ds(opp * CB, CB)], swst.at[0], D)
    sw_st_u = send(sw.at[pl.ds(2, 2), :, pl.ds(opp * CB, CB)], swst.at[1], U)
    here = swb.at[pl.ds(c * 4, 4), pl.ds(y * SF, SF), :]
    sw_u = send(sw.at[:, :, pl.ds(ym(1) * CB, CB)], here, U)
    sw_d = send(sw.at[:, :, pl.ds(ym(-1) * CB, CB)], here, D)

    def tw_part(k):
        rows = pl.ds(k * 512, 512)
        return send(tw.at[rows, :], twb.at[pl.ds(c * VB + k * 512, 512), :], mate)

    tw_in = [tw_part(0)]

    sh_own.wait()
    for d in s_y:
        d.wait_recv()

    def sblock(xx, lo=0, n=512):
        return sbuf.at[z, pl.ds(lo, n), pl.ds(xx * SF, SF)]

    sx_r = send(sblock(x), sblock(x), R)
    sx_l = send(sblock(x), sblock(x), L)

    @pl.when(x != y)
    def _():
        th_move.wait_recv()

    @pl.when(x == y)
    def _():
        th_own.wait()

    tx = {}

    def send_x(off):
        zz = zm(off)
        tx[1, off] = send(tshard(0, zz), tshard(1, zz), R)
        tx[2, off] = send(tshard(0, zz), tshard(2, zz), L)

    tz_f = send(tshard(0, z), tshard(0, z), F)
    tz_b = send(tshard(0, z), tshard(0, z), B)
    send_x(0)
    for k in (1, 2, 3):
        tw_in.append(tw_part(k))
        tz_f.wait_recv()
        if k < 3:
            nf = send(tshard(0, zm(-k)), tshard(0, zm(-k)), F)
        else:
            nf = send(tshard(0, zm(-k), 0, 64), tshard(0, zm(-k), 0, 64), F)
        tz_b.wait_recv()
        if k < 3:
            nb = send(tshard(0, zm(k)), tshard(0, zm(k)), B)
        else:
            nb = send(tshard(0, zm(k), 64, 64), tshard(0, zm(k), 64, 64), B)
        tz_f, tz_b = nf, nb
        send_x(-k)
        send_x(k)
        if k == 1:
            sx_r.wait_recv()
            sx_fr = send(sblock(xm(-1), 0, 256), sblock(xm(-1), 0, 256), R)
            sx_l.wait_recv()
            sx_fl = send(sblock(xm(1), 256, 256), sblock(xm(1), 256, 256), L)
        if k == 2:
            sw_st_d.wait_recv()
            src = ym(1)
            sw_fd = send(swst.at[0], swb.at[pl.ds(c * 4, 2), pl.ds(src * SF, SF), :], D)
            sw_st_u.wait_recv()
            src = ym(-1)
            sw_fu = send(swst.at[1], swb.at[pl.ds(c * 4 + 2, 2), pl.ds(src * SF, SF), :], U)
    tz_f.wait_recv()
    tz_b.wait_recv()
    send_x(4)

    sx_fr.wait_recv()
    sx_fl.wait_recv()

    def sz_block(zz, lo=0, n=512):
        return sbuf.at[zz, pl.ds(lo, n), :]

    sz = {}
    sz["f"] = send(sz_block(z), sz_block(z), F)
    sz["b"] = send(sz_block(z), sz_block(z), B)

    def sz_step(k):
        n, lo = (512, 0) if k < 3 else (256, 256)
        sz["f"].wait_recv()
        sz["f"] = send(sz_block(zm(-k), 0, n), sz_block(zm(-k), 0, n), F)
        sz["b"].wait_recv()
        sz["b"] = send(sz_block(zm(k), lo, n), sz_block(zm(k), lo, n), B)

    def forward_r(off):
        tx[1, off].wait_recv()
        zz = zm(off)
        tx[3, off] = send(tshard(1, zz), tshard(3, zz), R)

    def forward_l(off):
        tx[2, off].wait_recv()
        zz = zm(off)
        tx[3, off] = send(tshard(2, zz), tshard(3, zz), L)

    targets = (ym(2), ym(-1), ym(1), y)

    def product(stage, q0, q1):
        lo, m = STAGES[stage]

        def step(i, carry):
            q = lax.div(i, 2)
            h = lax.rem(i, 2)
            tgt = lax.rem(y + jnp.where(q == 0, 2, jnp.where(q == 1, 3, jnp.where(q == 2, 1, 0))), NY)
            cols = pl.ds(pl.multiple_of(tgt * CB + h * 256, 256), 256)
            pbuf[q, lo : lo + m, pl.ds(pl.multiple_of(h * 256, 256), 256)] = jnp.dot(
                tbuf[lo : lo + m, :], twb[:, cols], preferred_element_type=F32
            )
            return carry

        lax.fori_loop(2 * q0, 2 * q1, step, 0)

    rs = {}

    def halves(stage):
        lo, m = STAGES[stage]
        return pl.ds(lo, m // 2), pl.ds(lo + m // 2, m // 2)

    def send_opp(stage):
        a, b = halves(stage)
        rs[stage, "oa"] = send(pbuf.at[0, a, :], ropp.at[a, :], D)
        rs[stage, "ob"] = send(pbuf.at[0, b, :], ropp.at[b, :], U)

    def send_plain(stage):
        a, b = halves(stage)
        rs[stage, "pb"] = send(pbuf.at[1, b, :], rfin.at[0, b, :], D)
        rs[stage, "pa"] = send(pbuf.at[2, a, :], rfin.at[1, a, :], U)

    def send_sums(stage):
        a, b = halves(stage)
        lo, m = STAGES[stage]
        h = m // 2
        rs[stage, "oa"].wait_recv()
        pbuf[1, lo : lo + h, :] += ropp[lo : lo + h, :]
        rs[stage, "sa"] = send(pbuf.at[1, a, :], rfin.at[0, a, :], D)
        rs[stage, "ob"].wait_recv()
        pbuf[2, lo + h : lo + m, :] += ropp[lo + h : lo + m, :]
        rs[stage, "sb"] = send(pbuf.at[2, b, :], rfin.at[1, b, :], U)

    def teacher_stage(stage):
        product(stage, 0, 1)
        send_opp(stage)
        product(stage, 1, 4)
        send_plain(stage)

    for off in OFFS[:4]:
        forward_r(off)
    tw_own.wait()
    for d in tw_in:
        d.wait_recv()
    teacher_stage(0)
    for off in OFFS[4:]:
        forward_l(off)
    send_sums(0)
    sz_step(1)
    for off in OFFS[4:]:
        tx[1, off].wait_recv()
    for off in OFFS[:4]:
        tx[2, off].wait_recv()
    teacher_stage(1)

    sw_own.wait()
    sw_mate = []

    def to_mate(src, first, n):
        part = swb.at[pl.ds(c * 4 + first, n), pl.ds(src * SF, SF), :]
        sw_mate.append(send(part, part, mate))

    to_mate(y, 0, 4)
    sw_u.wait_recv()
    to_mate(ym(-1), 0, 4)
    sw_d.wait_recv()
    to_mate(ym(1), 0, 4)
    sw_fd.wait_recv()
    sw_fu.wait_recv()
    to_mate(ym(2), 0, 4)

    send_sums(1)
    sz_step(2)
    for off in OFFS:
        tx[3, off].wait_recv()
    teacher_stage(2)
    for d in sw_mate:
        d.wait_recv()
    send_sums(2)
    sz_step(3)

    def student(off_lo, off_hi, first):
        def step(i, carry):
            zz = lax.rem(z + i, NZ)
            part = jnp.dot(sbuf[zz], swb[zz], preferred_element_type=F32)
            slog[...] += part
            return carry

        if first:
            slog[...] = jnp.zeros_like(slog)
        lax.fori_loop(off_lo, off_hi, step, 0)

    student(5, 12, True)
    sz["f"].wait_recv()
    sz["b"].wait_recv()
    student(4, 5, False)

    for stage in range(3):
        for name in ("pb", "pa", "sa", "sb"):
            rs[stage, name].wait_recv()

    lane = lax.broadcasted_iota(jnp.int32, (TOK, 128), 1)

    def token_stats(slot, carry):
        group = lax.rem(x + jnp.where(slot == 1, 3, jnp.where(slot == 2, 1, jnp.where(slot == 3, 2, 0))), NX)
        rows = pl.ds(pl.multiple_of(slot * TOK, TOK), TOK)
        t = pbuf[3, rows, :] + rfin[0, rows, :] + rfin[1, rows, :]
        s = slog[pl.ds(pl.multiple_of(group * TOK, TOK), TOK), :]
        t_top = jnp.max(t, axis=1, keepdims=True)
        s_top = jnp.max(s, axis=1, keepdims=True)
        e = jnp.exp(t - t_top)
        t_sum = jnp.sum(e, axis=1, keepdims=True)
        w = jnp.sum(e * (t - s), axis=1, keepdims=True)
        s_sum = jnp.sum(jnp.exp(s - s_top), axis=1, keepdims=True)
        both = jnp.where(
            lane == 0, t_top,
            jnp.where(lane == 1, t_sum, jnp.where(lane == 2, w, jnp.where(lane == 3, s_top, s_sum))),
        )
        stat[group] = jnp.transpose(both)[:8, :]
        return carry

    lax.fori_loop(0, 4, token_stats, 0)

    def merged(ref, n):
        parts = [ref[k] for k in range(n)]
        t_top = parts[0][0:1]
        s_top = parts[0][3:4]
        for p in parts[1:]:
            t_top = jnp.maximum(t_top, p[0:1])
            s_top = jnp.maximum(s_top, p[3:4])
        t_sum = w = s_sum = jnp.zeros((1, 128), F32)
        for p in parts:
            a = jnp.exp(p[0:1] - t_top)
            b = jnp.exp(p[3:4] - s_top)
            t_sum += p[1:2] * a
            w += p[2:3] * a
            s_sum += p[4:5] * b
        return t_top, t_sum, w, s_top, s_sum

    def put(ref, k, rows):
        zero = jnp.zeros((3, 128), F32)
        ref[k] = jnp.concatenate([*rows, zero], axis=0)

    st1[y] = stat[y]
    got = [send(stat.at[ym(d)], st1.at[y], dev(x, ym(d), z, c)) for d in range(1, NY)]
    for d in got:
        d.wait_recv()
    put(st2, x, merged(st1, NY))
    got = [send(st2.at[x], st2.at[x], dev(xm(d), y, z, c)) for d in range(1, NX)]
    for d in got:
        d.wait_recv()
    put(st3, z, merged(st2, NX))
    got = [send(st3.at[z], st3.at[z], dev(x, y, zm(d), c)) for d in range(1, NZ)]
    for d in got:
        d.wait_recv()
    t_top, t_sum, w, s_top, s_sum = merged(st3, NZ)
    kl = w / t_sum - (t_top + jnp.log(t_sum)) + (s_top + jnp.log(s_sum))
    kl_ref[...] = kl
    st4[dp] = jnp.broadcast_to(jnp.sum(kl, axis=1, keepdims=True), (8, 128))
    got = [send(st4.at[dp], st4.at[dp], (lax.rem(dp + d, 8), v)) for d in range(1, 8)]
    for d in got:
        d.wait_recv()
    total = st4[0]
    for k in range(1, 8):
        total += st4[k]
    loss_ref[...] = total * (1.0 / (TOK * 8))

    for d in started:
        d.wait_send()

    @pl.when(x != y)
    def _():
        th_move.wait_send()

    assert count[0] == N_REMOTE, count[0]


def shards(th, sh, tw, sw):
    hbm = pl.BlockSpec(memory_space=pl.ANY)
    vmem = pl.BlockSpec(memory_space=pltpu.VMEM)
    bf16 = jnp.bfloat16
    kl, loss = pl.pallas_call(
        body,
        out_shape=(
            jax.ShapeDtypeStruct((1, TOK), F32),
            jax.ShapeDtypeStruct((8, 128), F32),
        ),
        in_specs=[hbm] * 4,
        out_specs=(vmem, vmem),
        scratch_shapes=[
            pltpu.VMEM((4 * TOK, NZ * TF), bf16),
            pltpu.VMEM((NZ, 4 * TOK, NX * SF), bf16),
            pltpu.VMEM((2 * VB, VB), bf16),
            pltpu.VMEM((NZ, NX * SF, CB), bf16),
            pltpu.VMEM((2, 2, SF, CB), bf16),
            pltpu.VMEM((4, 4 * TOK, CB), F32),
            pltpu.VMEM((4 * TOK, CB), F32),
            pltpu.VMEM((2, 4 * TOK, CB), F32),
            pltpu.VMEM((4 * TOK, CB), F32),
            pltpu.VMEM((NY, 8, 128), F32),
            pltpu.VMEM((NY, 8, 128), F32),
            pltpu.VMEM((NX, 8, 128), F32),
            pltpu.VMEM((NZ, 8, 128), F32),
            pltpu.VMEM((8, 8, 128), F32),
            pltpu.SemaphoreType.DMA((N_REMOTE,)),
            pltpu.SemaphoreType.DMA((N_REMOTE,)),
            pltpu.SemaphoreType.DMA((4,)),
        ],
        compiler_params=pltpu.CompilerParams(
            collective_id=0, has_side_effects=True, vmem_limit_bytes=60 * 1024 * 1024
        ),
        name="kl_all",
    )(th, sh, tw, sw.reshape(4, SF, VB))
    return (kl.reshape(TOK), loss[0, 0])


def solution(mesh):
    in_specs = (P("dp", "vocab"),) * 4
    return jax.shard_map(
        shards, mesh=mesh, in_specs=in_specs, out_specs=(P("dp"), P()), check_vma=False
    )
```

```python
import math

import jax
import jax.numpy as jnp
from jax import lax
from jax.experimental import pallas as pl
from jax.experimental.pallas import tpu as pltpu
from jax.sharding import PartitionSpec as P

NX, NY, NZ = 4, 4, 8
TOK = 128
HALF = TOK // 2
TF = 512
SF = 128
VB = 2048
CB = VB // NY
F32 = jnp.float32

OWN, LEFT, RIGHT, OPP = (0, 64), (128, 256), (192, 320), (384, 448)
N_STAGES = 4
AR = 384
BR = 4 * TOK - AR
N_SEND, N_RECV = 15, 74


def body(
    th, sh, tw, sw,
    kl_ref, loss_ref,
    tst, tbuf, sbuf, twb, swb, swst, pbuf, ropp, rfin, slog, stat, st1, st3, st4, kl_v, loss_v,
    ssem, rsem, lsem,
):
    dp = lax.axis_index("dp")
    v = lax.axis_index("vocab")
    y, c = lax.div(dp, 2), lax.rem(dp, 2)
    x, z = lax.div(v, NZ), lax.rem(v, NZ)
    o = 1 - c

    def dev(xx, yy, zz, cc):
        return (yy * 2 + cc, xx * NZ + zz)

    def xm(d):
        return lax.rem(x + (d + NX), NX)

    def ym(d):
        return lax.rem(y + (d + NY), NY)

    def zm(d):
        return lax.rem(z + (d + NZ), NZ)

    R, L = dev(xm(1), y, z, c), dev(xm(-1), y, z, c)
    U, D = dev(x, ym(1), z, c), dev(x, ym(-1), z, c)
    F, B = dev(x, y, zm(1), c), dev(x, y, zm(-1), c)
    mate = dev(x, y, z, o)

    s_index, r_index = {}, {}
    s_bytes, r_bytes = {}, {}

    def nbytes(ref):
        return math.prod(ref.shape) * jnp.dtype(ref.dtype).itemsize

    def remote(src, dst, device, sgroup, rgroup):
        i = s_index.setdefault(sgroup, len(s_index))
        j = r_index.setdefault(rgroup, len(r_index))
        s_bytes[sgroup] = s_bytes.get(sgroup, 0) + nbytes(src)
        r_bytes[rgroup] = r_bytes.get(rgroup, 0) + nbytes(dst)
        return pltpu.make_async_remote_copy(
            src_ref=src,
            dst_ref=dst,
            send_sem=ssem.at[i],
            recv_sem=rsem.at[j],
            device_id=device,
            device_id_type=pl.DeviceIdType.MESH,
        )

    def send(src, dst, device, sgroup, rgroup):
        remote(src, dst, device, sgroup, rgroup).start()

    def awaiting(ref, i, j):
        return pltpu.make_async_remote_copy(
            src_ref=ref,
            dst_ref=ref,
            send_sem=ssem.at[i],
            recv_sem=rsem.at[j],
            device_id=mate,
            device_id_type=pl.DeviceIdType.MESH,
        )

    def arrived(rgroup, ref):
        assert r_bytes.pop(rgroup) == nbytes(ref), rgroup
        awaiting(ref, 0, r_index[rgroup]).wait_recv()

    def sent(sgroup, ref):
        assert s_bytes.pop(sgroup) == nbytes(ref), sgroup
        awaiting(ref, s_index[sgroup], 0).wait_send()

    th_in = pltpu.make_async_copy(th, tst, lsem.at[4])
    th_in.start()
    sh_here = sbuf.at[z, pl.ds(y * TOK, TOK), pl.ds(x * SF, SF)]
    sh_own = pltpu.make_async_copy(sh, sh_here, lsem.at[2])
    sh_own.start()

    def tshard(row, zz, n=HALF):
        return tbuf.at[pl.ds(row, n), pl.ds(zz * TF, TF)]

    stays = jnp.logical_and(c == 0, x == y)
    moves = jnp.logical_or(c == 1, x != y)
    th_own = pltpu.make_async_copy(th, tshard(0, z, TOK), lsem.at[3])

    @pl.when(stays)
    def _():
        th_own.start()

    tw_own = pltpu.make_async_copy(tw, twb.at[pl.ds(c * VB, VB), :], lsem.at[0])
    tw_own.start()
    sw_own = pltpu.make_async_copy(
        sw.at[:, :, pl.ds(y * CB, CB)], swb.at[pl.ds(c * 4, 4), pl.ds(y * SF, SF), :], lsem.at[1]
    )
    sw_own.start()

    barrier = pltpu.get_barrier_semaphore()
    peers = [dev(xm(d), y, z, c) for d in (1, -1)]
    peers += [dev(x, ym(d), z, c) for d in (1, -1, 2)]
    peers += [dev(x, y, zm(d), c) for d in (1, -1)]
    peers += [mate]
    for p in peers:
        pl.semaphore_signal(barrier, inc=1, device_id=p, device_id_type=pl.DeviceIdType.MESH)

    @pl.when(moves)
    def _():
        source = dev(y, lax.rem(x + 2 * c, NY), z, c)
        pl.semaphore_signal(barrier, inc=1, device_id=source, device_id_type=pl.DeviceIdType.MESH)
        pl.semaphore_wait(barrier, len(peers) + 1)

    @pl.when(stays)
    def _():
        pl.semaphore_wait(barrier, len(peers))

    th_in.wait()
    sh_own.wait()
    th_move = remote(tst, tshard(0, z, TOK), dev(lax.rem(y + 2 * c, NX), x, z, c), "th", "th")

    @pl.when(moves)
    def _():
        th_move.start()

    for d in (1, -1, 2):
        send(sh_here, sh_here, dev(x, ym(d), z, c), "sy", "sy")

    opp = ym(2)
    send(sw.at[pl.ds(0, 2), :, pl.ds(opp * CB, CB)], swst.at[0], D, "sw", "swst0")
    send(sw.at[pl.ds(2, 2), :, pl.ds(opp * CB, CB)], swst.at[1], U, "sw", "swst1")

    def sw_rows(src, first, n):
        return swb.at[pl.ds(c * 4 + first, n), pl.ds(src * SF, SF), :]

    send(sw.at[:, :, pl.ds(ym(1) * CB, CB)], sw_rows(y, 0, 4), U, "sw", "sw_u")
    send(sw.at[:, :, pl.ds(ym(-1) * CB, CB)], sw_rows(y, 0, 4), D, "sw", "sw_d")

    def forward_sw():
        arrived("swst0", swst.at[0])
        send(swst.at[0], sw_rows(ym(1), 0, 2), D, "sw", "swf")
        arrived("swst1", swst.at[1])
        send(swst.at[1], sw_rows(ym(-1), 2, 2), U, "sw", "swf")

    for k in range(4):
        send(tw.at[pl.ds(k * 512, 512), :], twb.at[pl.ds(c * VB + k * 512, 512), :], mate, "tw", "tw")

    @pl.when(moves)
    def _():
        th_move.wait_recv()

    @pl.when(stays)
    def _():
        th_own.wait()

    def tz_send(way, off, h):
        part = tshard(HALF * h, zm(off))
        send(part, part, F if way == "f" else B, "tz", ("tz", way, abs(off) + 1, h))

    def tz_arrived(way, k, h):
        arrived(("tz", way, k, h), tshard(HALF * h, z))

    def tx_first(off):
        zz = zm(off)
        send(tshard(OWN[0], zz), tshard(LEFT[0], zz), R, "tx", "L0")
        send(tshard(OWN[0], zz), tshard(RIGHT[0], zz), L, "tx", "R0")

    def rows64(row, part=None):
        cols = pl.ds(0, NZ * TF) if part is None else pl.ds(part * 4 * TF, 4 * TF)
        return tbuf.at[pl.ds(row, HALF), cols]

    for h in (0, 1):
        tz_send("f", 0, h)
        tz_send("b", 0, h)

    def sx_rows(xx, lo=0, n=AR):
        return sbuf.at[z, pl.ds(lo, n), pl.ds(xx * SF, SF)]

    arrived("sy", sbuf.at[0, pl.ds(0, 3 * TOK), pl.ds(0, SF)])
    send(sx_rows(x), sx_rows(x), R, "sx", "sxr")
    send(sx_rows(x), sx_rows(x), L, "sx", "sxl")
    tx_first(0)

    def forward_sx():
        h = AR // 2
        arrived("sxr", sx_rows(x))
        send(sx_rows(xm(-1), 0, h), sx_rows(xm(-1), 0, h), R, "sx", "sxfr")
        arrived("sxl", sx_rows(x))
        send(sx_rows(xm(1), h, h), sx_rows(xm(1), h, h), L, "sx", "sxfl")

    for k in (1, 2, 3):
        for h in (0, 1):
            tz_arrived("f", k, h)
            if k < 3 or h == 0:
                tz_send("f", -k, h)
            tz_arrived("b", k, h)
            if k < 3 or h == 1:
                tz_send("b", k, h)
        if k == 2:
            forward_sx()
        tx_first(-k)
        tx_first(k)
        if k == 2:
            forward_sw()
    tz_arrived("f", 4, 0)
    tx_first(4)
    tz_arrived("b", 4, 1)
    for part in (0, 1):
        send(rows64(OWN[1], part), rows64(LEFT[1], part), R, "tx", "L1")
        send(rows64(OWN[1], part), rows64(RIGHT[1], part), L, "tx", ("R1", part))

    def sz_send(way, off, h):
        part = sbuf.at[zm(off), pl.ds(AR // 2 * h, AR // 2), :]
        send(part, part, F if way == "f" else B, "sz", ("sz", way, abs(off) + 1, h))

    def sz_arrived(way, k, h):
        arrived(("sz", way, k, h), sbuf.at[z, pl.ds(0, AR // 2), :])

    def sz_step(k, h):
        sz_arrived("f", k, h)
        if k < 3 or h == 0:
            sz_send("f", -k, h)
        sz_arrived("b", k, h)
        if k < 3 or h == 1:
            sz_send("b", k, h)

    def sb_send(way, off, lo=AR, n=BR):
        part = sbuf.at[zm(off), pl.ds(lo, n), pl.ds(x * SF, SF)]
        send(part, part, F if way == "f" else B, "sb", ("sb", way, abs(off) + 1))

    def sb_step(k):
        for way, sign, lo in (("f", -1, AR), ("b", 1, AR + BR // 2)):
            arrived(("sb", way, k), sbuf.at[z, pl.ds(AR, BR), pl.ds(0, SF)])
            sb_send(way, sign * k) if k < 3 else sb_send(way, sign * k, lo, BR // 2)

    def sb_rows(xx, z0=0, nz=NZ):
        return sbuf.at[pl.ds(z0, nz), pl.ds(AR, BR), pl.ds(xx * SF, SF)]

    def sbx_send():
        for way in ("f", "b"):
            arrived(("sb", way, 4), sbuf.at[z, pl.ds(AR, BR // 2), pl.ds(0, SF)])
        send(sb_rows(x), sb_rows(x), R, "sbx", "sbr")
        send(sb_rows(x), sb_rows(x), L, "sbx", "sbl")

    def forward_sbx():
        arrived("sbr", sb_rows(x))
        send(sb_rows(xm(-1), 0, 4), sb_rows(xm(-1), 0, 4), R, "sbx", "sbf")
        arrived("sbl", sb_rows(x))
        send(sb_rows(xm(1), 4, 4), sb_rows(xm(1), 4, 4), L, "sbx", "sbf")

    def start_sz():
        sb_send("f", 0)
        sb_send("b", 0)
        arrived("sxfr", sx_rows(x, 0, AR // 2))
        sz_send("f", 0, 0)
        sz_send("b", 0, 0)
        arrived("sxfl", sx_rows(x, 0, AR // 2))
        sz_send("f", 0, 1)
        sz_send("b", 0, 1)

    def product(stage, q0, q1):
        lo = stage * TOK

        def step(i, carry):
            q = lax.div(i, 2)
            h = lax.rem(i, 2)
            tgt = lax.rem(y + jnp.where(q == 0, 2, jnp.where(q == 1, 3, jnp.where(q == 2, 1, 0))), NY)
            cols = pl.ds(pl.multiple_of(tgt * CB + h * 256, 256), 256)
            pbuf[q, lo : lo + TOK, pl.ds(pl.multiple_of(h * 256, 256), 256)] = jnp.dot(
                tbuf[lo : lo + TOK, :], twb[:, cols], preferred_element_type=F32
            )
            return carry

        lax.fori_loop(2 * q0, 2 * q1, step, 0)

    def halves(stage):
        return pl.ds(stage * TOK, HALF), pl.ds(stage * TOK + HALF, HALF)

    def send_opp(stage):
        a, b = halves(stage)
        send(pbuf.at[0, a, :], ropp.at[a, :], D, "rs", ("oa", stage))
        send(pbuf.at[0, b, :], ropp.at[b, :], U, "rs", ("ob", stage))

    def send_plain(stage):
        a, b = halves(stage)
        send(pbuf.at[1, b, :], rfin.at[0, b, :], D, "rs", ("fin", stage))
        send(pbuf.at[2, a, :], rfin.at[1, a, :], U, "rs", ("fin", stage))

    def send_sums(stage):
        a, b = halves(stage)
        lo = stage * TOK
        mid, hi = lo + HALF, lo + TOK
        arrived(("oa", stage), ropp.at[a, :])
        pbuf[1, lo:mid, :] += ropp[lo:mid, :]
        send(pbuf.at[1, a, :], rfin.at[0, a, :], D, "rs", ("fin", stage))
        arrived(("ob", stage), ropp.at[b, :])
        pbuf[2, mid:hi, :] += ropp[mid:hi, :]
        send(pbuf.at[2, b, :], rfin.at[1, b, :], U, "rs", ("fin", stage))

    def teacher_stage(stage, between):
        product(stage, 0, 1)
        send_opp(stage)
        between()
        product(stage, 1, 4)
        send_plain(stage)

    def to_mate(src):
        send(sw_rows(src, 0, 4), sw_rows(src, 0, 4), mate, "mate", "mate")

    def student(first, last, lo=0, n=AR):
        def step(i, carry):
            zz = lax.rem(z + i, NZ)
            slog[lo : lo + n, :] += jnp.dot(
                sbuf[zz, lo : lo + n, :], swb[zz], preferred_element_type=F32
            )
            return carry

        lax.fori_loop(first, last, step, 0)

    tw_own.wait()
    arrived("tw", twb.at[pl.ds(0, VB), :])
    teacher_stage(0, start_sz)

    arrived("L0", rows64(LEFT[0]))
    send(rows64(LEFT[0]), rows64(OPP[0]), R, "tx", "O0")
    arrived("R0", rows64(RIGHT[0]))

    def stage_one():
        send_sums(0)
        sb_step(1)

    teacher_stage(1, stage_one)

    sw_own.wait()
    to_mate(y)
    arrived("sw_u", sw_rows(y, 0, 4))
    to_mate(ym(-1))
    arrived("sw_d", sw_rows(y, 0, 4))
    to_mate(ym(1))

    sz_step(1, 0)
    sb_step(2)
    send_sums(1)
    sz_step(1, 1)
    for part in (0, 1):
        arrived(("R1", part), rows64(RIGHT[1], 0))
        send(rows64(RIGHT[1], part), rows64(OPP[1], part), L, "tx", "O1")
    arrived("L1", rows64(LEFT[1]))
    teacher_stage(2, lambda: sb_step(3))
    arrived("swf", sw_rows(y, 0, 4))
    to_mate(ym(2))
    sz_step(2, 0)
    send_sums(2)
    sz_step(2, 1)
    sbx_send()
    arrived("O0", rows64(OPP[0]))
    arrived("O1", rows64(OPP[1]))
    teacher_stage(3, lambda: sz_step(3, 0))
    slog[...] = jnp.zeros_like(slog)
    arrived("mate", swb.at[pl.ds(0, 4)])
    student(6, 11)
    sz_step(3, 1)
    forward_sbx()
    send_sums(3)
    student(5, 6)
    student(3, 4)
    sz_arrived("f", 4, 0)
    sz_arrived("b", 4, 1)
    student(4, 5)
    arrived("sbf", sb_rows(x))
    student(0, NZ, AR, BR)

    sent("sy", sbuf.at[0, pl.ds(0, 3 * TOK), pl.ds(0, SF)])
    sent("sx", sbuf.at[0, pl.ds(0, 288), :])
    sent("tz", tbuf.at[pl.ds(0, 112), :])
    sent("tx", tbuf.at[pl.ds(0, 384), :])
    sent("sz", sbuf.at[pl.ds(0, 7), pl.ds(0, AR), :])
    sent("sb", sbuf.at[0, pl.ds(0, 224), :])
    sent("sbx", sbuf.at[pl.ds(0, 2), pl.ds(0, 384), :])
    sent("sw", swb.at[pl.ds(0, 4)])
    sent("mate", swb.at[pl.ds(0, 4)])
    sent("tw", twb.at[pl.ds(0, VB), :])

    @pl.when(moves)
    def _():
        th_move.wait_send()

    lane = lax.broadcasted_iota(jnp.int32, (TOK, 128), 1)

    def token_stats(first_rows, ahead):
        group = lax.rem(x + 2 * c + ahead, NY)

        def rows(ref, *at):
            return jnp.concatenate([ref[(*at, slice(r, r + HALF))] for r in first_rows], axis=0)

        t = rows(pbuf, 3) + rows(rfin, 0) + rows(rfin, 1)
        s = slog[pl.ds(pl.multiple_of(group * TOK, TOK), TOK), :]
        t_top = jnp.max(t, axis=1, keepdims=True)
        s_top = jnp.max(s, axis=1, keepdims=True)
        e = jnp.exp(t - t_top)
        t_sum = jnp.sum(e, axis=1, keepdims=True)
        w = jnp.sum(e * (t - s), axis=1, keepdims=True)
        s_sum = jnp.sum(jnp.exp(s - s_top), axis=1, keepdims=True)
        both = jnp.where(
            lane == 0, t_top,
            jnp.where(lane == 1, t_sum, jnp.where(lane == 2, w, jnp.where(lane == 3, s_top, s_sum))),
        )
        stat[group] = jnp.transpose(both)[:8, :]

    def stage_done(stage):
        arrived(("fin", stage), rfin.at[0, pl.ds(0, 2 * TOK), :])

    stage_done(0)
    token_stats(OWN, 0)
    stage_done(1)
    stage_done(2)
    token_stats(LEFT, 3)
    token_stats(RIGHT, 1)
    stage_done(3)
    token_stats(OPP, 2)

    def merged(ref, n):
        parts = [ref[k] for k in range(n)]
        t_top = parts[0][0:1]
        s_top = parts[0][3:4]
        for p in parts[1:]:
            t_top = jnp.maximum(t_top, p[0:1])
            s_top = jnp.maximum(s_top, p[3:4])
        t_sum = w = s_sum = jnp.zeros((1, 128), F32)
        for p in parts:
            a = jnp.exp(p[0:1] - t_top)
            b = jnp.exp(p[3:4] - s_top)
            t_sum += p[1:2] * a
            w += p[2:3] * a
            s_sum += p[4:5] * b
        return t_top, t_sum, w, s_top, s_sum

    def put(ref, k, rows):
        zero = jnp.zeros((3, 128), F32)
        ref[k] = jnp.concatenate([*rows, zero], axis=0)

    me = x * NY + y
    st1[me] = stat[y]
    for dy in range(NY):
        for dx in range(NX):
            if dx or dy:
                send(stat.at[ym(dy)], st1.at[me], dev(xm(dx), ym(dy), z, c), "st1", "st1")
    sent("rs", pbuf.at[pl.ds(0, 3)])
    arrived("st1", st1.at[pl.ds(0, NX * NY - 1)])
    put(st3, z, merged(st1, NX * NY))
    for d in range(1, NZ):
        send(st3.at[z], st3.at[z], dev(x, y, zm(d), c), "st3", "st3")
    sent("st1", st1.at[pl.ds(0, NX * NY - 1)])
    arrived("st3", st3.at[pl.ds(0, NZ - 1)])
    t_top, t_sum, w, s_top, s_sum = merged(st3, NZ)
    kl = w / t_sum - (t_top + jnp.log(t_sum)) + (s_top + jnp.log(s_sum))
    st4[dp] = jnp.broadcast_to(jnp.sum(kl, axis=1, keepdims=True), (8, 128))
    for d in range(1, 8):
        send(st4.at[dp], st4.at[dp], (lax.rem(dp + d, 8), v), "st4", "st4")
    kl_v[...] = kl
    kl_out = pltpu.make_async_copy(kl_v, kl_ref, lsem.at[5])
    kl_out.start()
    sent("st3", st3.at[pl.ds(0, NZ - 1)])
    arrived("st4", st4.at[pl.ds(0, 7)])
    total = st4[0]
    for k in range(1, 8):
        total += st4[k]
    loss_v[...] = total[0:1] * (1.0 / (TOK * 8))
    loss_out = pltpu.make_async_copy(loss_v, loss_ref, lsem.at[6])
    loss_out.start()
    sent("st4", st4.at[pl.ds(0, 7)])
    kl_out.wait()
    loss_out.wait()
    assert set(s_bytes) == {"th"} and set(r_bytes) == {"th"}, (s_bytes, r_bytes)
    assert (len(s_index), len(r_index)) == (N_SEND, N_RECV), (len(s_index), len(r_index))


def shards(th, sh, tw, sw):
    hbm = pl.BlockSpec(memory_space=pl.ANY)
    bf16 = jnp.bfloat16
    kl, loss = pl.pallas_call(
        body,
        out_shape=(
            jax.ShapeDtypeStruct((1, TOK), F32),
            jax.ShapeDtypeStruct((1, 128), F32),
        ),
        in_specs=[hbm] * 4,
        out_specs=(hbm, hbm),
        scratch_shapes=[
            pltpu.VMEM((TOK, TF), bf16),
            pltpu.VMEM((4 * TOK, NZ * TF), bf16),
            pltpu.VMEM((NZ, 4 * TOK, NX * SF), bf16),
            pltpu.VMEM((2 * VB, VB), bf16),
            pltpu.VMEM((NZ, NX * SF, CB), bf16),
            pltpu.VMEM((2, 2, SF, CB), bf16),
            pltpu.VMEM((4, 4 * TOK, CB), F32),
            pltpu.VMEM((4 * TOK, CB), F32),
            pltpu.VMEM((2, 4 * TOK, CB), F32),
            pltpu.VMEM((4 * TOK, CB), F32),
            pltpu.VMEM((NY, 8, 128), F32),
            pltpu.VMEM((NX * NY, 8, 128), F32),
            pltpu.VMEM((NZ, 8, 128), F32),
            pltpu.VMEM((8, 8, 128), F32),
            pltpu.VMEM((1, TOK), F32),
            pltpu.VMEM((1, 128), F32),
            pltpu.SemaphoreType.DMA((N_SEND,)),
            pltpu.SemaphoreType.DMA((N_RECV,)),
            pltpu.SemaphoreType.DMA((7,)),
        ],
        compiler_params=pltpu.CompilerParams(
            collective_id=0, has_side_effects=True, vmem_limit_bytes=60 * 1024 * 1024
        ),
        name="kl_all",
    )(th, sh, tw, sw.reshape(4, SF, VB))
    return (kl.reshape(TOK), loss[0, 0])


def solution(mesh):
    in_specs = (P("dp", "vocab"),) * 4
    return jax.shard_map(
        shards, mesh=mesh, in_specs=in_specs, out_specs=(P("dp"), P()), check_vma=False
    )
```

```python
import math

import jax
import jax.numpy as jnp
from jax import lax
from jax.experimental import pallas as pl
from jax.experimental.pallas import tpu as pltpu
from jax.sharding import PartitionSpec as P

NX, NY, NZ = 4, 4, 8
TOK = 128
HALF = TOK // 2
TF = 512
SF = 128
VB = 2048
CB = VB // NY
F32 = jnp.float32

OWN, LEFT, RIGHT, OPP = (0, 64), (128, 256), (192, 320), (384, 448)
N_STAGES = 4
AR = 384
BR = 4 * TOK - AR
N_SEND, N_RECV = 15, 74


def body(
    th, sh, tw, sw,
    kl_ref, loss_ref,
    tst, tbuf, sbuf, twb, swb, swst, pbuf, ropp, rfin, slog, stat, st1, st3, st4, kl_v, loss_v,
    ssem, rsem, lsem,
):
    dp = lax.axis_index("dp")
    v = lax.axis_index("vocab")
    y, c = lax.div(dp, 2), lax.rem(dp, 2)
    x, z = lax.div(v, NZ), lax.rem(v, NZ)
    o = 1 - c

    def dev(xx, yy, zz, cc):
        return (yy * 2 + cc, xx * NZ + zz)

    def xm(d):
        return lax.rem(x + (d + NX), NX)

    def ym(d):
        return lax.rem(y + (d + NY), NY)

    def zm(d):
        return lax.rem(z + (d + NZ), NZ)

    R, L = dev(xm(1), y, z, c), dev(xm(-1), y, z, c)
    U, D = dev(x, ym(1), z, c), dev(x, ym(-1), z, c)
    F, B = dev(x, y, zm(1), c), dev(x, y, zm(-1), c)
    mate = dev(x, y, z, o)

    s_index, r_index = {}, {}
    s_bytes, r_bytes = {}, {}

    def nbytes(ref):
        return math.prod(ref.shape) * jnp.dtype(ref.dtype).itemsize

    def remote(src, dst, device, sgroup, rgroup):
        i = s_index.setdefault(sgroup, len(s_index))
        j = r_index.setdefault(rgroup, len(r_index))
        s_bytes[sgroup] = s_bytes.get(sgroup, 0) + nbytes(src)
        r_bytes[rgroup] = r_bytes.get(rgroup, 0) + nbytes(dst)
        return pltpu.make_async_remote_copy(
            src_ref=src,
            dst_ref=dst,
            send_sem=ssem.at[i],
            recv_sem=rsem.at[j],
            device_id=device,
            device_id_type=pl.DeviceIdType.MESH,
        )

    def send(src, dst, device, sgroup, rgroup):
        remote(src, dst, device, sgroup, rgroup).start()

    def awaiting(ref, i, j):
        return pltpu.make_async_remote_copy(
            src_ref=ref,
            dst_ref=ref,
            send_sem=ssem.at[i],
            recv_sem=rsem.at[j],
            device_id=mate,
            device_id_type=pl.DeviceIdType.MESH,
        )

    def arrived(rgroup, ref):
        assert r_bytes.pop(rgroup) == nbytes(ref), rgroup
        awaiting(ref, 0, r_index[rgroup]).wait_recv()

    def sent(sgroup, ref):
        assert s_bytes.pop(sgroup) == nbytes(ref), sgroup
        awaiting(ref, s_index[sgroup], 0).wait_send()

    th_in = pltpu.make_async_copy(th, tst, lsem.at[4])
    th_in.start()
    sh_here = sbuf.at[z, pl.ds(y * TOK, TOK), pl.ds(x * SF, SF)]
    sh_own = pltpu.make_async_copy(sh, sh_here, lsem.at[2])
    sh_own.start()

    def tshard(row, zz, n=HALF):
        return tbuf.at[pl.ds(row, n), pl.ds(zz * TF, TF)]

    stays = jnp.logical_and(c == 0, x == y)
    moves = jnp.logical_or(c == 1, x != y)
    th_own = pltpu.make_async_copy(th, tshard(0, z, TOK), lsem.at[3])

    @pl.when(stays)
    def _():
        th_own.start()

    tw_own = pltpu.make_async_copy(tw, twb.at[pl.ds(c * VB, VB), :], lsem.at[0])
    tw_own.start()
    sw_own = pltpu.make_async_copy(
        sw.at[:, :, pl.ds(y * CB, CB)], swb.at[pl.ds(c * 4, 4), pl.ds(y * SF, SF), :], lsem.at[1]
    )
    sw_own.start()

    barrier = pltpu.get_barrier_semaphore()
    peers = [dev(xm(d), y, z, c) for d in (1, -1)]
    peers += [dev(x, ym(d), z, c) for d in (1, -1, 2)]
    peers += [dev(x, y, zm(d), c) for d in (1, -1)]
    peers += [mate]
    for p in peers:
        pl.semaphore_signal(barrier, inc=1, device_id=p, device_id_type=pl.DeviceIdType.MESH)

    @pl.when(moves)
    def _():
        source = dev(y, lax.rem(x + 2 * c, NY), z, c)
        pl.semaphore_signal(barrier, inc=1, device_id=source, device_id_type=pl.DeviceIdType.MESH)
        pl.semaphore_wait(barrier, len(peers) + 1)

    @pl.when(stays)
    def _():
        pl.semaphore_wait(barrier, len(peers))

    th_in.wait()
    sh_own.wait()
    th_move = remote(tst, tshard(0, z, TOK), dev(lax.rem(y + 2 * c, NX), x, z, c), "th", "th")

    @pl.when(moves)
    def _():
        th_move.start()

    for d in (1, -1, 2):
        send(sh_here, sh_here, dev(x, ym(d), z, c), "sy", "sy")

    opp = ym(2)
    send(sw.at[pl.ds(0, 2), :, pl.ds(opp * CB, CB)], swst.at[0], D, "sw", "swst0")
    send(sw.at[pl.ds(2, 2), :, pl.ds(opp * CB, CB)], swst.at[1], U, "sw", "swst1")

    def sw_rows(src, first, n):
        return swb.at[pl.ds(c * 4 + first, n), pl.ds(src * SF, SF), :]

    send(sw.at[:, :, pl.ds(ym(1) * CB, CB)], sw_rows(y, 0, 4), U, "sw", "sw_u")
    send(sw.at[:, :, pl.ds(ym(-1) * CB, CB)], sw_rows(y, 0, 4), D, "sw", "sw_d")

    def forward_sw():
        arrived("swst0", swst.at[0])
        send(swst.at[0], sw_rows(ym(1), 0, 2), D, "sw", "swf")
        arrived("swst1", swst.at[1])
        send(swst.at[1], sw_rows(ym(-1), 2, 2), U, "sw", "swf")

    for k in range(4):
        send(tw.at[pl.ds(k * 512, 512), :], twb.at[pl.ds(c * VB + k * 512, 512), :], mate, "tw", "tw")

    def sb_send(way, off, lo=AR, n=BR):
        part = sbuf.at[zm(off), pl.ds(lo, n), pl.ds(x * SF, SF)]
        send(part, part, F if way == "f" else B, "sb", ("sb", way, abs(off) + 1))

    def sb_step(k):
        for way, sign, lo in (("f", -1, AR), ("b", 1, AR + BR // 2)):
            arrived(("sb", way, k), sbuf.at[z, pl.ds(AR, BR), pl.ds(0, SF)])
            sb_send(way, sign * k) if k < 3 else sb_send(way, sign * k, lo, BR // 2)

    def sb_rows(xx, z0=0, nz=NZ):
        return sbuf.at[pl.ds(z0, nz), pl.ds(AR, BR), pl.ds(xx * SF, SF)]

    def sbx_send():
        for way in ("f", "b"):
            arrived(("sb", way, 4), sbuf.at[z, pl.ds(AR, BR // 2), pl.ds(0, SF)])
        send(sb_rows(x), sb_rows(x), R, "sbx", "sbr")
        send(sb_rows(x), sb_rows(x), L, "sbx", "sbl")

    def forward_sbx():
        arrived("sbr", sb_rows(x))
        send(sb_rows(xm(-1), 0, 4), sb_rows(xm(-1), 0, 4), R, "sbx", "sbf")
        arrived("sbl", sb_rows(x))
        send(sb_rows(xm(1), 4, 4), sb_rows(xm(1), 4, 4), L, "sbx", "sbf")

    @pl.when(moves)
    def _():
        th_move.wait_recv()

    @pl.when(stays)
    def _():
        th_own.wait()

    def tz_send(way, off, h):
        part = tshard(HALF * h, zm(off))
        send(part, part, F if way == "f" else B, "tz", ("tz", way, abs(off) + 1, h))

    def tz_arrived(way, k, h):
        arrived(("tz", way, k, h), tshard(HALF * h, z))

    def tx_first(off):
        zz = zm(off)
        send(tshard(OWN[0], zz), tshard(LEFT[0], zz), R, "tx", "L0")
        send(tshard(OWN[0], zz), tshard(RIGHT[0], zz), L, "tx", "R0")

    def rows64(row, part=None):
        cols = pl.ds(0, NZ * TF) if part is None else pl.ds(part * 4 * TF, 4 * TF)
        return tbuf.at[pl.ds(row, HALF), cols]

    for h in (0, 1):
        tz_send("f", 0, h)
        tz_send("b", 0, h)

    def sx_rows(xx, lo=0, n=AR):
        return sbuf.at[z, pl.ds(lo, n), pl.ds(xx * SF, SF)]

    arrived("sy", sbuf.at[0, pl.ds(0, 3 * TOK), pl.ds(0, SF)])
    sb_send("f", 0)
    sb_send("b", 0)
    send(sx_rows(x), sx_rows(x), R, "sx", "sxr")
    send(sx_rows(x), sx_rows(x), L, "sx", "sxl")
    tx_first(0)

    def forward_sx():
        h = AR // 2
        arrived("sxr", sx_rows(x))
        send(sx_rows(xm(-1), 0, h), sx_rows(xm(-1), 0, h), R, "sx", "sxfr")
        arrived("sxl", sx_rows(x))
        send(sx_rows(xm(1), h, h), sx_rows(xm(1), h, h), L, "sx", "sxfl")

    for k in (1, 2, 3):
        for h in (0, 1):
            tz_arrived("f", k, h)
            if k < 3 or h == 0:
                tz_send("f", -k, h)
            tz_arrived("b", k, h)
            if k < 3 or h == 1:
                tz_send("b", k, h)
        if k == 2:
            forward_sx()
        tx_first(-k)
        tx_first(k)
        sb_step(k)
        if k == 2:
            forward_sw()
    tz_arrived("f", 4, 0)
    tx_first(4)
    tz_arrived("b", 4, 1)
    for part in (0, 1):
        send(rows64(OWN[1], part), rows64(LEFT[1], part), R, "tx", "L1")
        send(rows64(OWN[1], part), rows64(RIGHT[1], part), L, "tx", ("R1", part))

    def sz_send(way, off, h):
        part = sbuf.at[zm(off), pl.ds(AR // 2 * h, AR // 2), :]
        send(part, part, F if way == "f" else B, "sz", ("sz", way, abs(off) + 1, h))

    def sz_arrived(way, k, h):
        arrived(("sz", way, k, h), sbuf.at[z, pl.ds(0, AR // 2), :])

    def sz_step(k, h):
        sz_arrived("f", k, h)
        if k < 3 or h == 0:
            sz_send("f", -k, h)
        sz_arrived("b", k, h)
        if k < 3 or h == 1:
            sz_send("b", k, h)

    def start_sz():
        arrived("sxfr", sx_rows(x, 0, AR // 2))
        sz_send("f", 0, 0)
        sz_send("b", 0, 0)
        arrived("sxfl", sx_rows(x, 0, AR // 2))
        sz_send("f", 0, 1)
        sz_send("b", 0, 1)

    def product(stage, q0, q1):
        lo = stage * TOK

        def step(i, carry):
            q = lax.div(i, 2)
            h = lax.rem(i, 2)
            tgt = lax.rem(y + jnp.where(q == 0, 2, jnp.where(q == 1, 3, jnp.where(q == 2, 1, 0))), NY)
            cols = pl.ds(pl.multiple_of(tgt * CB + h * 256, 256), 256)
            pbuf[q, lo : lo + TOK, pl.ds(pl.multiple_of(h * 256, 256), 256)] = jnp.dot(
                tbuf[lo : lo + TOK, :], twb[:, cols], preferred_element_type=F32
            )
            return carry

        lax.fori_loop(2 * q0, 2 * q1, step, 0)

    def halves(stage):
        return pl.ds(stage * TOK, HALF), pl.ds(stage * TOK + HALF, HALF)

    def send_opp(stage):
        a, b = halves(stage)
        send(pbuf.at[0, a, :], ropp.at[a, :], D, "rs", ("oa", stage))
        send(pbuf.at[0, b, :], ropp.at[b, :], U, "rs", ("ob", stage))

    def send_plain(stage):
        a, b = halves(stage)
        send(pbuf.at[1, b, :], rfin.at[0, b, :], D, "rs", ("fin", stage))
        send(pbuf.at[2, a, :], rfin.at[1, a, :], U, "rs", ("fin", stage))

    def send_sums(stage):
        a, b = halves(stage)
        lo = stage * TOK
        mid, hi = lo + HALF, lo + TOK
        arrived(("oa", stage), ropp.at[a, :])
        pbuf[1, lo:mid, :] += ropp[lo:mid, :]
        send(pbuf.at[1, a, :], rfin.at[0, a, :], D, "rs", ("fin", stage))
        arrived(("ob", stage), ropp.at[b, :])
        pbuf[2, mid:hi, :] += ropp[mid:hi, :]
        send(pbuf.at[2, b, :], rfin.at[1, b, :], U, "rs", ("fin", stage))

    def to_mate(src):
        send(sw_rows(src, 0, 4), sw_rows(src, 0, 4), mate, "mate", "mate")

    def student(first, last, lo=0, n=AR):
        def step(i, carry):
            zz = lax.rem(z + i, NZ)
            slog[lo : lo + n, :] += jnp.dot(
                sbuf[zz, lo : lo + n, :], swb[zz], preferred_element_type=F32
            )
            return carry

        lax.fori_loop(first, last, step, 0)

    tw_own.wait()
    arrived("tw", twb.at[pl.ds(0, VB), :])
    product(0, 0, 1)
    send_opp(0)
    start_sz()
    product(0, 1, 4)
    send_plain(0)

    arrived("L0", rows64(LEFT[0]))
    send(rows64(LEFT[0]), rows64(OPP[0]), R, "tx", "O0")
    arrived("R0", rows64(RIGHT[0]))
    product(1, 0, 1)
    send_opp(1)
    product(1, 1, 2)
    sz_step(1, 0)
    product(1, 2, 3)

    def forward_right(part):
        arrived(("R1", part), rows64(RIGHT[1], 0))
        send(rows64(RIGHT[1], part), rows64(OPP[1], part), L, "tx", "O1")

    send_sums(0)
    forward_right(0)
    product(1, 3, 4)
    send_plain(1)

    sw_own.wait()
    to_mate(y)
    arrived("sw_u", sw_rows(y, 0, 4))
    to_mate(ym(-1))
    arrived("sw_d", sw_rows(y, 0, 4))
    to_mate(ym(1))

    sz_step(1, 1)
    forward_right(1)
    sbx_send()
    arrived("L1", rows64(LEFT[1]))
    product(2, 0, 1)
    send_opp(2)
    send_sums(1)
    product(2, 1, 2)
    sz_step(2, 0)
    product(2, 2, 4)
    send_plain(2)
    arrived("swf", sw_rows(y, 0, 4))
    to_mate(ym(2))
    sz_step(2, 1)
    send_sums(2)
    slog[...] = jnp.zeros_like(slog)
    arrived("mate", swb.at[pl.ds(0, 4)])
    student(6, 11)
    arrived("O0", rows64(OPP[0]))
    arrived("O1", rows64(OPP[1]))
    product(3, 0, 1)
    send_opp(3)
    sz_step(3, 0)
    product(3, 1, 4)
    send_plain(3)
    sz_step(3, 1)
    forward_sbx()
    send_sums(3)
    student(5, 6)
    student(3, 4)
    sz_arrived("f", 4, 0)
    sz_arrived("b", 4, 1)
    student(4, 5)
    arrived("sbf", sb_rows(x))
    student(0, NZ, AR, BR)

    sent("sy", sbuf.at[0, pl.ds(0, 3 * TOK), pl.ds(0, SF)])
    sent("sx", sbuf.at[0, pl.ds(0, 288), :])
    sent("tz", tbuf.at[pl.ds(0, 112), :])
    sent("tx", tbuf.at[pl.ds(0, 384), :])
    sent("sz", sbuf.at[pl.ds(0, 7), pl.ds(0, AR), :])
    sent("sb", sbuf.at[0, pl.ds(0, 224), :])
    sent("sbx", sbuf.at[pl.ds(0, 2), pl.ds(0, 384), :])
    sent("sw", swb.at[pl.ds(0, 4)])
    sent("mate", swb.at[pl.ds(0, 4)])
    sent("tw", twb.at[pl.ds(0, VB), :])

    @pl.when(moves)
    def _():
        th_move.wait_send()

    lane = lax.broadcasted_iota(jnp.int32, (TOK, 128), 1)

    def token_stats(first_rows, ahead):
        group = lax.rem(x + 2 * c + ahead, NY)

        def rows(ref, *at):
            return jnp.concatenate([ref[(*at, slice(r, r + HALF))] for r in first_rows], axis=0)

        t = rows(pbuf, 3) + rows(rfin, 0) + rows(rfin, 1)
        s = slog[pl.ds(pl.multiple_of(group * TOK, TOK), TOK), :]
        t_top = jnp.max(t, axis=1, keepdims=True)
        s_top = jnp.max(s, axis=1, keepdims=True)
        e = jnp.exp(t - t_top)
        t_sum = jnp.sum(e, axis=1, keepdims=True)
        w = jnp.sum(e * (t - s), axis=1, keepdims=True)
        s_sum = jnp.sum(jnp.exp(s - s_top), axis=1, keepdims=True)
        both = jnp.where(
            lane == 0, t_top,
            jnp.where(lane == 1, t_sum, jnp.where(lane == 2, w, jnp.where(lane == 3, s_top, s_sum))),
        )
        stat[group] = jnp.transpose(both)[:8, :]

    def stage_done(stage):
        arrived(("fin", stage), rfin.at[0, pl.ds(0, 2 * TOK), :])

    stage_done(0)
    token_stats(OWN, 0)
    stage_done(1)
    stage_done(2)
    token_stats(LEFT, 3)
    token_stats(RIGHT, 1)
    stage_done(3)
    token_stats(OPP, 2)

    def merged(ref, n):
        parts = [ref[k] for k in range(n)]
        t_top = parts[0][0:1]
        s_top = parts[0][3:4]
        for p in parts[1:]:
            t_top = jnp.maximum(t_top, p[0:1])
            s_top = jnp.maximum(s_top, p[3:4])
        t_sum = w = s_sum = jnp.zeros((1, 128), F32)
        for p in parts:
            a = jnp.exp(p[0:1] - t_top)
            b = jnp.exp(p[3:4] - s_top)
            t_sum += p[1:2] * a
            w += p[2:3] * a
            s_sum += p[4:5] * b
        return t_top, t_sum, w, s_top, s_sum

    def put(ref, k, rows):
        zero = jnp.zeros((3, 128), F32)
        ref[k] = jnp.concatenate([*rows, zero], axis=0)

    me = x * NY + y
    st1[me] = stat[y]
    for dy in range(NY):
        for dx in range(NX):
            if dx or dy:
                send(stat.at[ym(dy)], st1.at[me], dev(xm(dx), ym(dy), z, c), "st1", "st1")
    sent("rs", pbuf.at[pl.ds(0, 3)])
    arrived("st1", st1.at[pl.ds(0, NX * NY - 1)])
    put(st3, z, merged(st1, NX * NY))
    for d in range(1, NZ):
        send(st3.at[z], st3.at[z], dev(x, y, zm(d), c), "st3", "st3")
    sent("st1", st1.at[pl.ds(0, NX * NY - 1)])
    arrived("st3", st3.at[pl.ds(0, NZ - 1)])
    t_top, t_sum, w, s_top, s_sum = merged(st3, NZ)
    kl = w / t_sum - (t_top + jnp.log(t_sum)) + (s_top + jnp.log(s_sum))
    st4[dp] = jnp.broadcast_to(jnp.sum(kl, axis=1, keepdims=True), (8, 128))
    for d in range(1, 8):
        send(st4.at[dp], st4.at[dp], (lax.rem(dp + d, 8), v), "st4", "st4")
    kl_v[...] = kl
    kl_out = pltpu.make_async_copy(kl_v, kl_ref, lsem.at[5])
    kl_out.start()
    sent("st3", st3.at[pl.ds(0, NZ - 1)])
    arrived("st4", st4.at[pl.ds(0, 7)])
    total = st4[0]
    for k in range(1, 8):
        total += st4[k]
    loss_v[...] = total * (1.0 / (TOK * 8))
    loss_out = pltpu.make_async_copy(loss_v, loss_ref, lsem.at[6])
    loss_out.start()
    sent("st4", st4.at[pl.ds(0, 7)])
    kl_out.wait()
    loss_out.wait()
    assert set(s_bytes) == {"th"} and set(r_bytes) == {"th"}, (s_bytes, r_bytes)
    assert (len(s_index), len(r_index)) == (N_SEND, N_RECV), (len(s_index), len(r_index))


def shards(th, sh, tw, sw):
    hbm = pl.BlockSpec(memory_space=pl.ANY)
    bf16 = jnp.bfloat16
    kl, loss = pl.pallas_call(
        body,
        out_shape=(
            jax.ShapeDtypeStruct((1, TOK), F32),
            jax.ShapeDtypeStruct((8, 128), F32),
        ),
        in_specs=[hbm] * 4,
        out_specs=(hbm, hbm),
        scratch_shapes=[
            pltpu.VMEM((TOK, TF), bf16),
            pltpu.VMEM((4 * TOK, NZ * TF), bf16),
            pltpu.VMEM((NZ, 4 * TOK, NX * SF), bf16),
            pltpu.VMEM((2 * VB, VB), bf16),
            pltpu.VMEM((NZ, NX * SF, CB), bf16),
            pltpu.VMEM((2, 2, SF, CB), bf16),
            pltpu.VMEM((4, 4 * TOK, CB), F32),
            pltpu.VMEM((4 * TOK, CB), F32),
            pltpu.VMEM((2, 4 * TOK, CB), F32),
            pltpu.VMEM((4 * TOK, CB), F32),
            pltpu.VMEM((NY, 8, 128), F32),
            pltpu.VMEM((NX * NY, 8, 128), F32),
            pltpu.VMEM((NZ, 8, 128), F32),
            pltpu.VMEM((8, 8, 128), F32),
            pltpu.VMEM((1, TOK), F32),
            pltpu.VMEM((8, 128), F32),
            pltpu.SemaphoreType.DMA((N_SEND,)),
            pltpu.SemaphoreType.DMA((N_RECV,)),
            pltpu.SemaphoreType.DMA((7,)),
        ],
        compiler_params=pltpu.CompilerParams(
            collective_id=0, has_side_effects=True, vmem_limit_bytes=60 * 1024 * 1024
        ),
        name="kl_all",
    )(th, sh, tw, sw.reshape(4, SF, VB))
    return (kl.reshape(TOK), loss[0, 0])


def solution(mesh):
    in_specs = (P("dp", "vocab"),) * 4
    return jax.shard_map(
        shards, mesh=mesh, in_specs=in_specs, out_specs=(P("dp"), P()), check_vma=False
    )
```

```python
import math

import jax
import jax.numpy as jnp
from jax import lax
from jax.experimental import pallas as pl
from jax.experimental.pallas import tpu as pltpu
from jax.sharding import PartitionSpec as P

NX, NY, NZ = 4, 4, 8
TOK = 128
HALF = TOK // 2
TF = 512
SF = 128
VB = 2048
CB = VB // NY
F32 = jnp.float32

OWN, LEFT, RIGHT, OPP = (0, 64), (128, 256), (192, 320), (384, 448)
N_STAGES = 4
AR = 384
BR = 4 * TOK - AR
N_SEND, N_RECV = 15, 74


def body(
    th, sh, tw, sw,
    kl_ref, loss_ref,
    tst, tbuf, sbuf, twb, swb, swst, pbuf, ropp, rfin, slog, stat, st1, st3, st4,
    ssem, rsem, lsem,
):
    dp = lax.axis_index("dp")
    v = lax.axis_index("vocab")
    y, c = lax.div(dp, 2), lax.rem(dp, 2)
    x, z = lax.div(v, NZ), lax.rem(v, NZ)
    o = 1 - c

    def dev(xx, yy, zz, cc):
        return (yy * 2 + cc, xx * NZ + zz)

    def xm(d):
        return lax.rem(x + (d + NX), NX)

    def ym(d):
        return lax.rem(y + (d + NY), NY)

    def zm(d):
        return lax.rem(z + (d + NZ), NZ)

    R, L = dev(xm(1), y, z, c), dev(xm(-1), y, z, c)
    U, D = dev(x, ym(1), z, c), dev(x, ym(-1), z, c)
    F, B = dev(x, y, zm(1), c), dev(x, y, zm(-1), c)
    mate = dev(x, y, z, o)

    s_index, r_index = {}, {}
    s_bytes, r_bytes = {}, {}

    def nbytes(ref):
        return math.prod(ref.shape) * jnp.dtype(ref.dtype).itemsize

    def remote(src, dst, device, sgroup, rgroup):
        i = s_index.setdefault(sgroup, len(s_index))
        j = r_index.setdefault(rgroup, len(r_index))
        s_bytes[sgroup] = s_bytes.get(sgroup, 0) + nbytes(src)
        r_bytes[rgroup] = r_bytes.get(rgroup, 0) + nbytes(dst)
        return pltpu.make_async_remote_copy(
            src_ref=src,
            dst_ref=dst,
            send_sem=ssem.at[i],
            recv_sem=rsem.at[j],
            device_id=device,
            device_id_type=pl.DeviceIdType.MESH,
        )

    def send(src, dst, device, sgroup, rgroup):
        remote(src, dst, device, sgroup, rgroup).start()

    def awaiting(ref, i, j):
        return pltpu.make_async_remote_copy(
            src_ref=ref,
            dst_ref=ref,
            send_sem=ssem.at[i],
            recv_sem=rsem.at[j],
            device_id=mate,
            device_id_type=pl.DeviceIdType.MESH,
        )

    def arrived(rgroup, ref):
        assert r_bytes.pop(rgroup) == nbytes(ref), rgroup
        awaiting(ref, 0, r_index[rgroup]).wait_recv()

    def sent(sgroup, ref):
        assert s_bytes.pop(sgroup) == nbytes(ref), sgroup
        awaiting(ref, s_index[sgroup], 0).wait_send()

    th_in = pltpu.make_async_copy(th, tst, lsem.at[4])
    th_in.start()
    sh_here = sbuf.at[z, pl.ds(y * TOK, TOK), pl.ds(x * SF, SF)]
    sh_own = pltpu.make_async_copy(sh, sh_here, lsem.at[2])
    sh_own.start()

    def tshard(row, zz, n=HALF):
        return tbuf.at[pl.ds(row, n), pl.ds(zz * TF, TF)]

    stays = jnp.logical_and(c == 0, x == y)
    moves = jnp.logical_or(c == 1, x != y)
    th_own = pltpu.make_async_copy(th, tshard(0, z, TOK), lsem.at[3])

    @pl.when(stays)
    def _():
        th_own.start()

    tw_own = pltpu.make_async_copy(tw, twb.at[pl.ds(c * VB, VB), :], lsem.at[0])
    tw_own.start()
    sw_own = pltpu.make_async_copy(
        sw.at[:, :, pl.ds(y * CB, CB)], swb.at[pl.ds(c * 4, 4), pl.ds(y * SF, SF), :], lsem.at[1]
    )
    sw_own.start()

    barrier = pltpu.get_barrier_semaphore()
    peers = [dev(xm(d), y, z, c) for d in (1, -1)]
    peers += [dev(x, ym(d), z, c) for d in (1, -1, 2)]
    peers += [dev(x, y, zm(d), c) for d in (1, -1)]
    peers += [mate]
    for p in peers:
        pl.semaphore_signal(barrier, inc=1, device_id=p, device_id_type=pl.DeviceIdType.MESH)

    @pl.when(moves)
    def _():
        source = dev(y, lax.rem(x + 2 * c, NY), z, c)
        pl.semaphore_signal(barrier, inc=1, device_id=source, device_id_type=pl.DeviceIdType.MESH)
        pl.semaphore_wait(barrier, len(peers) + 1)

    @pl.when(stays)
    def _():
        pl.semaphore_wait(barrier, len(peers))

    th_in.wait()
    sh_own.wait()
    th_move = remote(tst, tshard(0, z, TOK), dev(lax.rem(y + 2 * c, NX), x, z, c), "th", "th")

    @pl.when(moves)
    def _():
        th_move.start()

    for d in (1, -1, 2):
        send(sh_here, sh_here, dev(x, ym(d), z, c), "sy", "sy")

    opp = ym(2)
    send(sw.at[pl.ds(0, 2), :, pl.ds(opp * CB, CB)], swst.at[0], D, "sw", "swst0")
    send(sw.at[pl.ds(2, 2), :, pl.ds(opp * CB, CB)], swst.at[1], U, "sw", "swst1")

    def sw_rows(src, first, n):
        return swb.at[pl.ds(c * 4 + first, n), pl.ds(src * SF, SF), :]

    send(sw.at[:, :, pl.ds(ym(1) * CB, CB)], sw_rows(y, 0, 4), U, "sw", "sw_u")
    send(sw.at[:, :, pl.ds(ym(-1) * CB, CB)], sw_rows(y, 0, 4), D, "sw", "sw_d")

    def forward_sw():
        arrived("swst0", swst.at[0])
        send(swst.at[0], sw_rows(ym(1), 0, 2), D, "sw", "swf")
        arrived("swst1", swst.at[1])
        send(swst.at[1], sw_rows(ym(-1), 2, 2), U, "sw", "swf")

    for k in range(4):
        send(tw.at[pl.ds(k * 512, 512), :], twb.at[pl.ds(c * VB + k * 512, 512), :], mate, "tw", "tw")

    def sb_send(way, off, lo=AR, n=BR):
        part = sbuf.at[zm(off), pl.ds(lo, n), pl.ds(x * SF, SF)]
        send(part, part, F if way == "f" else B, "sb", ("sb", way, abs(off) + 1))

    def sb_step(k):
        for way, sign, lo in (("f", -1, AR), ("b", 1, AR + BR // 2)):
            arrived(("sb", way, k), sbuf.at[z, pl.ds(AR, BR), pl.ds(0, SF)])
            sb_send(way, sign * k) if k < 3 else sb_send(way, sign * k, lo, BR // 2)

    def sb_rows(xx, z0=0, nz=NZ):
        return sbuf.at[pl.ds(z0, nz), pl.ds(AR, BR), pl.ds(xx * SF, SF)]

    def sbx_send():
        for way in ("f", "b"):
            arrived(("sb", way, 4), sbuf.at[z, pl.ds(AR, BR // 2), pl.ds(0, SF)])
        send(sb_rows(x), sb_rows(x), R, "sbx", "sbr")
        send(sb_rows(x), sb_rows(x), L, "sbx", "sbl")

    def forward_sbx():
        arrived("sbr", sb_rows(x))
        send(sb_rows(xm(-1), 0, 4), sb_rows(xm(-1), 0, 4), R, "sbx", "sbf")
        arrived("sbl", sb_rows(x))
        send(sb_rows(xm(1), 4, 4), sb_rows(xm(1), 4, 4), L, "sbx", "sbf")

    @pl.when(moves)
    def _():
        th_move.wait_recv()

    @pl.when(stays)
    def _():
        th_own.wait()

    def tz_send(way, off, h):
        part = tshard(HALF * h, zm(off))
        send(part, part, F if way == "f" else B, "tz", ("tz", way, abs(off) + 1, h))

    def tz_arrived(way, k, h):
        arrived(("tz", way, k, h), tshard(HALF * h, z))

    def tx_first(off):
        zz = zm(off)
        send(tshard(OWN[0], zz), tshard(LEFT[0], zz), R, "tx", "L0")
        send(tshard(OWN[0], zz), tshard(RIGHT[0], zz), L, "tx", "R0")

    def rows64(row, part=None):
        cols = pl.ds(0, NZ * TF) if part is None else pl.ds(part * 4 * TF, 4 * TF)
        return tbuf.at[pl.ds(row, HALF), cols]

    for h in (0, 1):
        tz_send("f", 0, h)
        tz_send("b", 0, h)

    def sx_rows(xx, lo=0, n=AR):
        return sbuf.at[z, pl.ds(lo, n), pl.ds(xx * SF, SF)]

    arrived("sy", sbuf.at[0, pl.ds(0, 3 * TOK), pl.ds(0, SF)])
    sb_send("f", 0)
    sb_send("b", 0)
    send(sx_rows(x), sx_rows(x), R, "sx", "sxr")
    send(sx_rows(x), sx_rows(x), L, "sx", "sxl")
    tx_first(0)

    def forward_sx():
        h = AR // 2
        arrived("sxr", sx_rows(x))
        send(sx_rows(xm(-1), 0, h), sx_rows(xm(-1), 0, h), R, "sx", "sxfr")
        arrived("sxl", sx_rows(x))
        send(sx_rows(xm(1), h, h), sx_rows(xm(1), h, h), L, "sx", "sxfl")

    for k in (1, 2, 3):
        for h in (0, 1):
            tz_arrived("f", k, h)
            if k < 3 or h == 0:
                tz_send("f", -k, h)
            tz_arrived("b", k, h)
            if k < 3 or h == 1:
                tz_send("b", k, h)
        if k == 2:
            forward_sx()
        tx_first(-k)
        tx_first(k)
        sb_step(k)
        if k == 2:
            forward_sw()
    tz_arrived("f", 4, 0)
    tx_first(4)
    tz_arrived("b", 4, 1)
    for part in (0, 1):
        send(rows64(OWN[1], part), rows64(LEFT[1], part), R, "tx", "L1")
        send(rows64(OWN[1], part), rows64(RIGHT[1], part), L, "tx", ("R1", part))

    def sz_send(way, off, h):
        part = sbuf.at[zm(off), pl.ds(AR // 2 * h, AR // 2), :]
        send(part, part, F if way == "f" else B, "sz", ("sz", way, abs(off) + 1, h))

    def sz_arrived(way, k, h):
        arrived(("sz", way, k, h), sbuf.at[z, pl.ds(0, AR // 2), :])

    def sz_step(k, h):
        sz_arrived("f", k, h)
        if k < 3 or h == 0:
            sz_send("f", -k, h)
        sz_arrived("b", k, h)
        if k < 3 or h == 1:
            sz_send("b", k, h)

    def start_sz():
        arrived("sxfr", sx_rows(x, 0, AR // 2))
        sz_send("f", 0, 0)
        sz_send("b", 0, 0)
        arrived("sxfl", sx_rows(x, 0, AR // 2))
        sz_send("f", 0, 1)
        sz_send("b", 0, 1)

    def product(stage, q0, q1):
        lo = stage * TOK

        def step(i, carry):
            q = lax.div(i, 2)
            h = lax.rem(i, 2)
            tgt = lax.rem(y + jnp.where(q == 0, 2, jnp.where(q == 1, 3, jnp.where(q == 2, 1, 0))), NY)
            cols = pl.ds(pl.multiple_of(tgt * CB + h * 256, 256), 256)
            pbuf[q, lo : lo + TOK, pl.ds(pl.multiple_of(h * 256, 256), 256)] = jnp.dot(
                tbuf[lo : lo + TOK, :], twb[:, cols], preferred_element_type=F32
            )
            return carry

        lax.fori_loop(2 * q0, 2 * q1, step, 0)

    def halves(stage):
        return pl.ds(stage * TOK, HALF), pl.ds(stage * TOK + HALF, HALF)

    def send_opp(stage):
        a, b = halves(stage)
        send(pbuf.at[0, a, :], ropp.at[a, :], D, "rs", ("oa", stage))
        send(pbuf.at[0, b, :], ropp.at[b, :], U, "rs", ("ob", stage))

    def send_plain(stage):
        a, b = halves(stage)
        send(pbuf.at[1, b, :], rfin.at[0, b, :], D, "rs", ("fin", stage))
        send(pbuf.at[2, a, :], rfin.at[1, a, :], U, "rs", ("fin", stage))

    def send_sums(stage):
        a, b = halves(stage)
        lo = stage * TOK
        mid, hi = lo + HALF, lo + TOK
        arrived(("oa", stage), ropp.at[a, :])
        pbuf[1, lo:mid, :] += ropp[lo:mid, :]
        send(pbuf.at[1, a, :], rfin.at[0, a, :], D, "rs", ("fin", stage))
        arrived(("ob", stage), ropp.at[b, :])
        pbuf[2, mid:hi, :] += ropp[mid:hi, :]
        send(pbuf.at[2, b, :], rfin.at[1, b, :], U, "rs", ("fin", stage))

    def to_mate(src):
        send(sw_rows(src, 0, 4), sw_rows(src, 0, 4), mate, "mate", "mate")

    def student(first, last, lo=0, n=AR):
        def step(i, carry):
            zz = lax.rem(z + i, NZ)
            slog[lo : lo + n, :] += jnp.dot(
                sbuf[zz, lo : lo + n, :], swb[zz], preferred_element_type=F32
            )
            return carry

        lax.fori_loop(first, last, step, 0)

    tw_own.wait()
    arrived("tw", twb.at[pl.ds(0, VB), :])
    product(0, 0, 1)
    send_opp(0)
    start_sz()
    product(0, 1, 4)
    send_plain(0)

    arrived("L0", rows64(LEFT[0]))
    send(rows64(LEFT[0]), rows64(OPP[0]), R, "tx", "O0")
    arrived("R0", rows64(RIGHT[0]))
    product(1, 0, 1)
    send_opp(1)
    product(1, 1, 2)
    sz_step(1, 0)
    product(1, 2, 3)

    def forward_right(part):
        arrived(("R1", part), rows64(RIGHT[1], 0))
        send(rows64(RIGHT[1], part), rows64(OPP[1], part), L, "tx", "O1")

    send_sums(0)
    forward_right(0)
    product(1, 3, 4)
    send_plain(1)

    sw_own.wait()
    to_mate(y)
    arrived("sw_u", sw_rows(y, 0, 4))
    to_mate(ym(-1))
    arrived("sw_d", sw_rows(y, 0, 4))
    to_mate(ym(1))

    sz_step(1, 1)
    forward_right(1)
    sbx_send()
    arrived("L1", rows64(LEFT[1]))
    product(2, 0, 1)
    send_opp(2)
    send_sums(1)
    product(2, 1, 2)
    sz_step(2, 0)
    product(2, 2, 4)
    send_plain(2)
    arrived("swf", sw_rows(y, 0, 4))
    to_mate(ym(2))
    sz_step(2, 1)
    send_sums(2)
    slog[...] = jnp.zeros_like(slog)
    arrived("mate", swb.at[pl.ds(0, 4)])
    student(6, 11)
    arrived("O0", rows64(OPP[0]))
    arrived("O1", rows64(OPP[1]))
    product(3, 0, 1)
    send_opp(3)
    sz_step(3, 0)
    product(3, 1, 4)
    send_plain(3)
    sz_step(3, 1)
    forward_sbx()
    send_sums(3)
    student(5, 6)
    student(3, 4)
    arrived("sbf", sb_rows(x))
    student(0, NZ, AR, BR)
    sz_arrived("f", 4, 0)
    sz_arrived("b", 4, 1)
    student(4, 5)

    sent("sy", sbuf.at[0, pl.ds(0, 3 * TOK), pl.ds(0, SF)])
    sent("sx", sbuf.at[0, pl.ds(0, 288), :])
    sent("tz", tbuf.at[pl.ds(0, 112), :])
    sent("tx", tbuf.at[pl.ds(0, 384), :])
    sent("sz", sbuf.at[pl.ds(0, 7), pl.ds(0, AR), :])
    sent("sb", sbuf.at[0, pl.ds(0, 224), :])
    sent("sbx", sbuf.at[pl.ds(0, 2), pl.ds(0, 384), :])
    sent("sw", swb.at[pl.ds(0, 4)])
    sent("mate", swb.at[pl.ds(0, 4)])
    sent("tw", twb.at[pl.ds(0, VB), :])

    @pl.when(moves)
    def _():
        th_move.wait_send()

    lane = lax.broadcasted_iota(jnp.int32, (TOK, 128), 1)

    def token_stats(first_rows, ahead):
        group = lax.rem(x + 2 * c + ahead, NY)

        def rows(ref, *at):
            return jnp.concatenate([ref[(*at, slice(r, r + HALF))] for r in first_rows], axis=0)

        t = rows(pbuf, 3) + rows(rfin, 0) + rows(rfin, 1)
        s = slog[pl.ds(pl.multiple_of(group * TOK, TOK), TOK), :]
        t_top = jnp.max(t, axis=1, keepdims=True)
        s_top = jnp.max(s, axis=1, keepdims=True)
        e = jnp.exp(t - t_top)
        t_sum = jnp.sum(e, axis=1, keepdims=True)
        w = jnp.sum(e * (t - s), axis=1, keepdims=True)
        s_sum = jnp.sum(jnp.exp(s - s_top), axis=1, keepdims=True)
        both = jnp.where(
            lane == 0, t_top,
            jnp.where(lane == 1, t_sum, jnp.where(lane == 2, w, jnp.where(lane == 3, s_top, s_sum))),
        )
        stat[group] = jnp.transpose(both)[:8, :]

    def stage_done(stage):
        arrived(("fin", stage), rfin.at[0, pl.ds(0, 2 * TOK), :])

    stage_done(0)
    token_stats(OWN, 0)
    stage_done(1)
    stage_done(2)
    token_stats(LEFT, 3)
    token_stats(RIGHT, 1)
    stage_done(3)
    token_stats(OPP, 2)

    def merged(ref, n):
        parts = [ref[k] for k in range(n)]
        t_top = parts[0][0:1]
        s_top = parts[0][3:4]
        for p in parts[1:]:
            t_top = jnp.maximum(t_top, p[0:1])
            s_top = jnp.maximum(s_top, p[3:4])
        t_sum = w = s_sum = jnp.zeros((1, 128), F32)
        for p in parts:
            a = jnp.exp(p[0:1] - t_top)
            b = jnp.exp(p[3:4] - s_top)
            t_sum += p[1:2] * a
            w += p[2:3] * a
            s_sum += p[4:5] * b
        return t_top, t_sum, w, s_top, s_sum

    def put(ref, k, rows):
        zero = jnp.zeros((3, 128), F32)
        ref[k] = jnp.concatenate([*rows, zero], axis=0)

    me = x * NY + y
    st1[me] = stat[y]
    far = (2, 1, 3, 0)
    for dx, dy in sorted(((dx, dy) for dx in far for dy in far), key=lambda d: -sum(min(k, 4 - k) for k in d))[:-1]:
        send(stat.at[ym(dy)], st1.at[me], dev(xm(dx), ym(dy), z, c), "st1", "st1")
    sent("rs", pbuf.at[pl.ds(0, 3)])
    arrived("st1", st1.at[pl.ds(0, NX * NY - 1)])
    put(st3, z, merged(st1, NX * NY))
    for d in (4, 3, 5, 2, 6, 1, 7):
        send(st3.at[z], st3.at[z], dev(x, y, zm(d), c), "st3", "st3")
    sent("st1", st1.at[pl.ds(0, NX * NY - 1)])
    arrived("st3", st3.at[pl.ds(0, NZ - 1)])
    t_top, t_sum, w, s_top, s_sum = merged(st3, NZ)
    kl = w / t_sum - (t_top + jnp.log(t_sum)) + (s_top + jnp.log(s_sum))
    st4[dp] = jnp.broadcast_to(jnp.sum(kl, axis=1, keepdims=True), (8, 128))
    for d in (4, 5, 3, 2, 6, 7, 1):
        send(st4.at[dp], st4.at[dp], (lax.rem(dp + d, 8), v), "st4", "st4")
    kl_ref[...] = kl
    sent("st3", st3.at[pl.ds(0, NZ - 1)])
    arrived("st4", st4.at[pl.ds(0, 7)])
    total = st4[0]
    for k in range(1, 8):
        total += st4[k]
    loss_ref[...] = total * (1.0 / (TOK * 8))
    sent("st4", st4.at[pl.ds(0, 7)])
    assert set(s_bytes) == {"th"} and set(r_bytes) == {"th"}, (s_bytes, r_bytes)
    assert (len(s_index), len(r_index)) == (N_SEND, N_RECV), (len(s_index), len(r_index))


def hand_out(kl_in, loss_in, kl_ref, loss_ref):
    kl_ref[...] = kl_in[...]
    loss_ref[...] = loss_in[0:1, 0:1]


def shards(th, sh, tw, sw):
    hbm = pl.BlockSpec(memory_space=pl.ANY)
    vmem = pl.BlockSpec(memory_space=pltpu.VMEM)
    bf16 = jnp.bfloat16
    kl, loss = pl.pallas_call(
        body,
        out_shape=(
            pltpu.VMEM((1, TOK), F32),
            pltpu.VMEM((8, 128), F32),
        ),
        in_specs=[hbm] * 4,
        out_specs=(vmem, vmem),
        scratch_shapes=[
            pltpu.VMEM((TOK, TF), bf16),
            pltpu.VMEM((4 * TOK, NZ * TF), bf16),
            pltpu.VMEM((NZ, 4 * TOK, NX * SF), bf16),
            pltpu.VMEM((2 * VB, VB), bf16),
            pltpu.VMEM((NZ, NX * SF, CB), bf16),
            pltpu.VMEM((2, 2, SF, CB), bf16),
            pltpu.VMEM((4, 4 * TOK, CB), F32),
            pltpu.VMEM((4 * TOK, CB), F32),
            pltpu.VMEM((2, 4 * TOK, CB), F32),
            pltpu.VMEM((4 * TOK, CB), F32),
            pltpu.VMEM((NY, 8, 128), F32),
            pltpu.VMEM((NX * NY, 8, 128), F32),
            pltpu.VMEM((NZ, 8, 128), F32),
            pltpu.VMEM((8, 8, 128), F32),
            pltpu.SemaphoreType.DMA((N_SEND,)),
            pltpu.SemaphoreType.DMA((N_RECV,)),
            pltpu.SemaphoreType.DMA((5,)),
        ],
        compiler_params=pltpu.CompilerParams(
            collective_id=0, has_side_effects=True, vmem_limit_bytes=60 * 1024 * 1024
        ),
        name="kl_all",
    )(th, sh, tw, sw.reshape(4, SF, VB))
    vmem = pl.BlockSpec(memory_space=pltpu.VMEM)
    kl, loss = pl.pallas_call(
        hand_out,
        out_shape=(jax.ShapeDtypeStruct((1, TOK), F32), jax.ShapeDtypeStruct((1, 1), F32)),
        in_specs=[vmem] * 2,
        out_specs=(vmem, vmem),
        name="hand_out",
    )(*(pltpu.with_memory_space_constraint(a, pltpu.VMEM) for a in (kl, loss)))
    return (kl.reshape(TOK), loss.reshape(()))


def solution(mesh):
    in_specs = (P("dp", "vocab"),) * 4
    return jax.shard_map(
        shards, mesh=mesh, in_specs=in_specs, out_specs=(P("dp"), P()), check_vma=False
    )
```

```python
import math

import jax
import jax.numpy as jnp
from jax import lax
from jax.experimental import pallas as pl
from jax.experimental.pallas import tpu as pltpu
from jax.sharding import PartitionSpec as P

NX, NY, NZ = 4, 4, 8
TOK = 128
HALF = TOK // 2
TF = 512
SF = 128
VB = 2048
CB = VB // NY
F32 = jnp.float32

OWN, LEFT, RIGHT, OPP = (0, 64), (128, 256), (192, 320), (384, 448)
N_STAGES = 4
AR = 384
BR = 4 * TOK - AR
N_SEND, N_RECV = 15, 74


def body(
    th, sh, tw, sw,
    kl_ref, loss_ref,
    tst, tbuf, sbuf, twb, swb, swst, pbuf, ropp, rfin, slog, stat, st1, st3, st4,
    ssem, rsem, lsem,
):
    dp = lax.axis_index("dp")
    v = lax.axis_index("vocab")
    y, c = lax.div(dp, 2), lax.rem(dp, 2)
    x, z = lax.div(v, NZ), lax.rem(v, NZ)
    o = 1 - c

    def dev(xx, yy, zz, cc):
        return (yy * 2 + cc, xx * NZ + zz)

    def xm(d):
        return lax.rem(x + (d + NX), NX)

    def ym(d):
        return lax.rem(y + (d + NY), NY)

    def zm(d):
        return lax.rem(z + (d + NZ), NZ)

    R, L = dev(xm(1), y, z, c), dev(xm(-1), y, z, c)
    U, D = dev(x, ym(1), z, c), dev(x, ym(-1), z, c)
    F, B = dev(x, y, zm(1), c), dev(x, y, zm(-1), c)
    mate = dev(x, y, z, o)

    s_index, r_index = {}, {}
    s_bytes, r_bytes = {}, {}

    def nbytes(ref):
        return math.prod(ref.shape) * jnp.dtype(ref.dtype).itemsize

    def remote(src, dst, device, sgroup, rgroup):
        i = s_index.setdefault(sgroup, len(s_index))
        j = r_index.setdefault(rgroup, len(r_index))
        s_bytes[sgroup] = s_bytes.get(sgroup, 0) + nbytes(src)
        r_bytes[rgroup] = r_bytes.get(rgroup, 0) + nbytes(dst)
        return pltpu.make_async_remote_copy(
            src_ref=src,
            dst_ref=dst,
            send_sem=ssem.at[i],
            recv_sem=rsem.at[j],
            device_id=device,
            device_id_type=pl.DeviceIdType.MESH,
        )

    def send(src, dst, device, sgroup, rgroup):
        remote(src, dst, device, sgroup, rgroup).start()

    def awaiting(ref, i, j):
        return pltpu.make_async_remote_copy(
            src_ref=ref,
            dst_ref=ref,
            send_sem=ssem.at[i],
            recv_sem=rsem.at[j],
            device_id=mate,
            device_id_type=pl.DeviceIdType.MESH,
        )

    def arrived(rgroup, ref):
        assert r_bytes.pop(rgroup) == nbytes(ref), rgroup
        awaiting(ref, 0, r_index[rgroup]).wait_recv()

    def sent(sgroup, ref):
        assert s_bytes.pop(sgroup) == nbytes(ref), sgroup
        awaiting(ref, s_index[sgroup], 0).wait_send()

    th_in = pltpu.make_async_copy(th, tst, lsem.at[4])
    th_in.start()
    sh_here = sbuf.at[z, pl.ds(y * TOK, TOK), pl.ds(x * SF, SF)]
    sh_own = pltpu.make_async_copy(sh, sh_here, lsem.at[2])
    sh_own.start()

    def tshard(row, zz, n=HALF):
        return tbuf.at[pl.ds(row, n), pl.ds(zz * TF, TF)]

    stays = jnp.logical_and(c == 0, x == y)
    moves = jnp.logical_or(c == 1, x != y)
    th_own = pltpu.make_async_copy(th, tshard(0, z, TOK), lsem.at[3])

    @pl.when(stays)
    def _():
        th_own.start()

    tw_own = pltpu.make_async_copy(tw, twb.at[pl.ds(c * VB, VB), :], lsem.at[0])
    tw_own.start()
    sw_own = pltpu.make_async_copy(
        sw.at[:, :, pl.ds(y * CB, CB)], swb.at[pl.ds(c * 4, 4), pl.ds(y * SF, SF), :], lsem.at[1]
    )
    sw_own.start()

    barrier = pltpu.get_barrier_semaphore()
    peers = [dev(xm(d), y, z, c) for d in (1, -1)]
    peers += [dev(x, ym(d), z, c) for d in (1, -1, 2)]
    peers += [dev(x, y, zm(d), c) for d in (1, -1)]
    peers += [mate]
    for p in peers:
        pl.semaphore_signal(barrier, inc=1, device_id=p, device_id_type=pl.DeviceIdType.MESH)

    @pl.when(moves)
    def _():
        source = dev(y, lax.rem(x + 2 * c, NY), z, c)
        pl.semaphore_signal(barrier, inc=1, device_id=source, device_id_type=pl.DeviceIdType.MESH)
        pl.semaphore_wait(barrier, len(peers) + 1)

    @pl.when(stays)
    def _():
        pl.semaphore_wait(barrier, len(peers))

    th_in.wait()
    sh_own.wait()
    th_move = remote(tst, tshard(0, z, TOK), dev(lax.rem(y + 2 * c, NX), x, z, c), "th", "th")

    @pl.when(moves)
    def _():
        th_move.start()

    for d in (1, -1, 2):
        send(sh_here, sh_here, dev(x, ym(d), z, c), "sy", "sy")

    opp = ym(2)
    send(sw.at[pl.ds(0, 2), :, pl.ds(opp * CB, CB)], swst.at[0], D, "sw", "swst0")
    send(sw.at[pl.ds(2, 2), :, pl.ds(opp * CB, CB)], swst.at[1], U, "sw", "swst1")

    def sw_rows(src, first, n):
        return swb.at[pl.ds(c * 4 + first, n), pl.ds(src * SF, SF), :]

    send(sw.at[:, :, pl.ds(ym(1) * CB, CB)], sw_rows(y, 0, 4), U, "sw", "sw_u")
    send(sw.at[:, :, pl.ds(ym(-1) * CB, CB)], sw_rows(y, 0, 4), D, "sw", "sw_d")

    def forward_sw():
        arrived("swst0", swst.at[0])
        send(swst.at[0], sw_rows(ym(1), 0, 2), D, "sw", "swf")
        arrived("swst1", swst.at[1])
        send(swst.at[1], sw_rows(ym(-1), 2, 2), U, "sw", "swf")

    for k in range(4):
        send(tw.at[pl.ds(k * 512, 512), :], twb.at[pl.ds(c * VB + k * 512, 512), :], mate, "tw", "tw")

    def sb_send(way, off, lo=AR, n=BR):
        part = sbuf.at[zm(off), pl.ds(lo, n), pl.ds(x * SF, SF)]
        send(part, part, F if way == "f" else B, "sb", ("sb", way, abs(off) + 1))

    def sb_step(k):
        for way, sign, lo in (("f", -1, AR), ("b", 1, AR + BR // 2)):
            arrived(("sb", way, k), sbuf.at[z, pl.ds(AR, BR), pl.ds(0, SF)])
            sb_send(way, sign * k) if k < 3 else sb_send(way, sign * k, lo, BR // 2)

    def sb_rows(xx, z0=0, nz=NZ):
        return sbuf.at[pl.ds(z0, nz), pl.ds(AR, BR), pl.ds(xx * SF, SF)]

    def sbx_send():
        for way in ("f", "b"):
            arrived(("sb", way, 4), sbuf.at[z, pl.ds(AR, BR // 2), pl.ds(0, SF)])
        send(sb_rows(x), sb_rows(x), R, "sbx", "sbr")
        send(sb_rows(x), sb_rows(x), L, "sbx", "sbl")

    def forward_sbx():
        arrived("sbr", sb_rows(x))
        send(sb_rows(xm(-1), 0, 4), sb_rows(xm(-1), 0, 4), R, "sbx", "sbf")
        arrived("sbl", sb_rows(x))
        send(sb_rows(xm(1), 4, 4), sb_rows(xm(1), 4, 4), L, "sbx", "sbf")

    @pl.when(moves)
    def _():
        th_move.wait_recv()

    @pl.when(stays)
    def _():
        th_own.wait()

    def tz_send(way, off, h):
        part = tshard(HALF * h, zm(off))
        send(part, part, F if way == "f" else B, "tz", ("tz", way, abs(off) + 1, h))

    def tz_arrived(way, k, h):
        arrived(("tz", way, k, h), tshard(HALF * h, z))

    def tx_first(off):
        zz = zm(off)
        send(tshard(OWN[0], zz), tshard(LEFT[0], zz), R, "tx", "L0")
        send(tshard(OWN[0], zz), tshard(RIGHT[0], zz), L, "tx", "R0")

    def rows64(row, part=None):
        cols = pl.ds(0, NZ * TF) if part is None else pl.ds(part * 4 * TF, 4 * TF)
        return tbuf.at[pl.ds(row, HALF), cols]

    for h in (0, 1):
        tz_send("f", 0, h)
        tz_send("b", 0, h)

    def sx_rows(xx, lo=0, n=AR):
        return sbuf.at[z, pl.ds(lo, n), pl.ds(xx * SF, SF)]

    arrived("sy", sbuf.at[0, pl.ds(0, 3 * TOK), pl.ds(0, SF)])
    sb_send("f", 0)
    sb_send("b", 0)
    send(sx_rows(x), sx_rows(x), R, "sx", "sxr")
    send(sx_rows(x), sx_rows(x), L, "sx", "sxl")
    tx_first(0)

    def forward_sx():
        h = AR // 2
        arrived("sxr", sx_rows(x))
        send(sx_rows(xm(-1), 0, h), sx_rows(xm(-1), 0, h), R, "sx", "sxfr")
        arrived("sxl", sx_rows(x))
        send(sx_rows(xm(1), h, h), sx_rows(xm(1), h, h), L, "sx", "sxfl")

    for k in (1, 2, 3):
        for h in (0, 1):
            tz_arrived("f", k, h)
            if k < 3 or h == 0:
                tz_send("f", -k, h)
            tz_arrived("b", k, h)
            if k < 3 or h == 1:
                tz_send("b", k, h)
        if k == 2:
            forward_sx()
        tx_first(-k)
        tx_first(k)
        sb_step(k)
        if k == 2:
            forward_sw()
    tz_arrived("f", 4, 0)
    tx_first(4)
    tz_arrived("b", 4, 1)
    for part in (0, 1):
        send(rows64(OWN[1], part), rows64(LEFT[1], part), R, "tx", "L1")
        send(rows64(OWN[1], part), rows64(RIGHT[1], part), L, "tx", ("R1", part))

    def sz_send(way, off, h):
        part = sbuf.at[zm(off), pl.ds(AR // 2 * h, AR // 2), :]
        send(part, part, F if way == "f" else B, "sz", ("sz", way, abs(off) + 1, h))

    def sz_arrived(way, k, h):
        arrived(("sz", way, k, h), sbuf.at[z, pl.ds(0, AR // 2), :])

    def sz_step(k, h):
        sz_arrived("f", k, h)
        if k < 3 or h == 0:
            sz_send("f", -k, h)
        sz_arrived("b", k, h)
        if k < 3 or h == 1:
            sz_send("b", k, h)

    def start_sz():
        arrived("sxfr", sx_rows(x, 0, AR // 2))
        sz_send("f", 0, 0)
        sz_send("b", 0, 0)
        arrived("sxfl", sx_rows(x, 0, AR // 2))
        sz_send("f", 0, 1)
        sz_send("b", 0, 1)

    def product(stage, q0, q1):
        lo = stage * TOK

        def step(i, carry):
            q = lax.div(i, 2)
            h = lax.rem(i, 2)
            tgt = lax.rem(y + jnp.where(q == 0, 2, jnp.where(q == 1, 3, jnp.where(q == 2, 1, 0))), NY)
            cols = pl.ds(pl.multiple_of(tgt * CB + h * 256, 256), 256)
            pbuf[q, lo : lo + TOK, pl.ds(pl.multiple_of(h * 256, 256), 256)] = jnp.dot(
                tbuf[lo : lo + TOK, :], twb[:, cols], preferred_element_type=F32
            )
            return carry

        lax.fori_loop(2 * q0, 2 * q1, step, 0)

    def halves(stage):
        return pl.ds(stage * TOK, HALF), pl.ds(stage * TOK + HALF, HALF)

    def send_opp(stage):
        a, b = halves(stage)
        send(pbuf.at[0, a, :], ropp.at[a, :], D, "rs", ("oa", stage))
        send(pbuf.at[0, b, :], ropp.at[b, :], U, "rs", ("ob", stage))

    def send_down(stage):
        b = halves(stage)[1]
        send(pbuf.at[1, b, :], rfin.at[0, b, :], D, "rs", ("fin", stage))

    def send_up(stage):
        a = halves(stage)[0]
        send(pbuf.at[2, a, :], rfin.at[1, a, :], U, "rs", ("fin", stage))

    def products_left(stage):
        product(stage, 1, 2)
        send_down(stage)
        product(stage, 2, 3)
        send_up(stage)
        product(stage, 3, 4)

    def send_sums(stage):
        a, b = halves(stage)
        lo = stage * TOK
        mid, hi = lo + HALF, lo + TOK
        arrived(("oa", stage), ropp.at[a, :])
        pbuf[1, lo:mid, :] += ropp[lo:mid, :]
        send(pbuf.at[1, a, :], rfin.at[0, a, :], D, "rs", ("fin", stage))
        arrived(("ob", stage), ropp.at[b, :])
        pbuf[2, mid:hi, :] += ropp[mid:hi, :]
        send(pbuf.at[2, b, :], rfin.at[1, b, :], U, "rs", ("fin", stage))

    def to_mate(src):
        send(sw_rows(src, 0, 4), sw_rows(src, 0, 4), mate, "mate", "mate")

    def student(first, last, lo=0, n=AR):
        def step(i, carry):
            zz = lax.rem(z + i, NZ)
            slog[lo : lo + n, :] += jnp.dot(
                sbuf[zz, lo : lo + n, :], swb[zz], preferred_element_type=F32
            )
            return carry

        lax.fori_loop(first, last, step, 0)

    tw_own.wait()
    arrived("tw", twb.at[pl.ds(0, VB), :])
    product(0, 0, 1)
    send_opp(0)
    start_sz()
    products_left(0)

    arrived("L0", rows64(LEFT[0]))
    send(rows64(LEFT[0]), rows64(OPP[0]), R, "tx", "O0")
    arrived("R0", rows64(RIGHT[0]))
    product(1, 0, 1)
    send_opp(1)
    product(1, 1, 2)
    send_down(1)
    sz_step(1, 0)
    product(1, 2, 3)
    send_up(1)

    def forward_right(part):
        arrived(("R1", part), rows64(RIGHT[1], 0))
        send(rows64(RIGHT[1], part), rows64(OPP[1], part), L, "tx", "O1")

    send_sums(0)
    forward_right(0)
    product(1, 3, 4)

    sw_own.wait()
    to_mate(y)
    arrived("sw_u", sw_rows(y, 0, 4))
    to_mate(ym(-1))
    arrived("sw_d", sw_rows(y, 0, 4))
    to_mate(ym(1))

    sz_step(1, 1)
    forward_right(1)
    sbx_send()
    arrived("L1", rows64(LEFT[1]))
    product(2, 0, 1)
    send_opp(2)
    send_sums(1)
    product(2, 1, 2)
    send_down(2)
    sz_step(2, 0)
    product(2, 2, 3)
    send_up(2)
    product(2, 3, 4)
    arrived("swf", sw_rows(y, 0, 4))
    to_mate(ym(2))
    sz_step(2, 1)
    send_sums(2)
    slog[...] = jnp.zeros_like(slog)
    arrived("mate", swb.at[pl.ds(0, 4)])
    student(6, 11)
    arrived("O0", rows64(OPP[0]))
    arrived("O1", rows64(OPP[1]))
    product(3, 0, 1)
    send_opp(3)
    sz_step(3, 0)
    products_left(3)
    sz_step(3, 1)
    forward_sbx()
    send_sums(3)
    student(5, 6)
    student(3, 4)
    arrived("sbf", sb_rows(x))
    student(0, NZ, AR, BR)
    sz_arrived("f", 4, 0)
    sz_arrived("b", 4, 1)
    student(4, 5)

    sent("sy", sbuf.at[0, pl.ds(0, 3 * TOK), pl.ds(0, SF)])
    sent("sx", sbuf.at[0, pl.ds(0, 288), :])
    sent("tz", tbuf.at[pl.ds(0, 112), :])
    sent("tx", tbuf.at[pl.ds(0, 384), :])
    sent("sz", sbuf.at[pl.ds(0, 7), pl.ds(0, AR), :])
    sent("sb", sbuf.at[0, pl.ds(0, 224), :])
    sent("sbx", sbuf.at[pl.ds(0, 2), pl.ds(0, 384), :])
    sent("sw", swb.at[pl.ds(0, 4)])
    sent("mate", swb.at[pl.ds(0, 4)])
    sent("tw", twb.at[pl.ds(0, VB), :])

    @pl.when(moves)
    def _():
        th_move.wait_send()

    lane = lax.broadcasted_iota(jnp.int32, (TOK, 128), 1)

    def token_stats(first_rows, ahead):
        group = lax.rem(x + 2 * c + ahead, NY)

        def rows(ref, *at):
            return jnp.concatenate([ref[(*at, slice(r, r + HALF))] for r in first_rows], axis=0)

        t = rows(pbuf, 3) + rows(rfin, 0) + rows(rfin, 1)
        s = slog[pl.ds(pl.multiple_of(group * TOK, TOK), TOK), :]
        t_top = jnp.max(t, axis=1, keepdims=True)
        s_top = jnp.max(s, axis=1, keepdims=True)
        e = jnp.exp(t - t_top)
        t_sum = jnp.sum(e, axis=1, keepdims=True)
        w = jnp.sum(e * (t - s), axis=1, keepdims=True)
        s_sum = jnp.sum(jnp.exp(s - s_top), axis=1, keepdims=True)
        both = jnp.where(
            lane == 0, t_top,
            jnp.where(lane == 1, t_sum, jnp.where(lane == 2, w, jnp.where(lane == 3, s_top, s_sum))),
        )
        stat[group] = jnp.transpose(both)[:8, :]

    def stage_done(stage):
        arrived(("fin", stage), rfin.at[0, pl.ds(0, 2 * TOK), :])

    stage_done(0)
    token_stats(OWN, 0)
    stage_done(1)
    stage_done(2)
    token_stats(LEFT, 3)
    token_stats(RIGHT, 1)
    stage_done(3)
    token_stats(OPP, 2)

    def merged(ref, n):
        parts = [ref[k] for k in range(n)]
        t_top = parts[0][0:1]
        s_top = parts[0][3:4]
        for p in parts[1:]:
            t_top = jnp.maximum(t_top, p[0:1])
            s_top = jnp.maximum(s_top, p[3:4])
        t_sum = w = s_sum = jnp.zeros((1, 128), F32)
        for p in parts:
            a = jnp.exp(p[0:1] - t_top)
            b = jnp.exp(p[3:4] - s_top)
            t_sum += p[1:2] * a
            w += p[2:3] * a
            s_sum += p[4:5] * b
        return t_top, t_sum, w, s_top, s_sum

    def put(ref, k, rows):
        zero = jnp.zeros((3, 128), F32)
        ref[k] = jnp.concatenate([*rows, zero], axis=0)

    me = x * NY + y
    st1[me] = stat[y]
    far = (2, 1, 3, 0)
    for dx, dy in sorted(((dx, dy) for dx in far for dy in far), key=lambda d: -sum(min(k, 4 - k) for k in d))[:-1]:
        send(stat.at[ym(dy)], st1.at[me], dev(xm(dx), ym(dy), z, c), "st1", "st1")
    sent("rs", pbuf.at[pl.ds(0, 3)])
    arrived("st1", st1.at[pl.ds(0, NX * NY - 1)])
    put(st3, z, merged(st1, NX * NY))
    for d in (4, 3, 5, 2, 6, 1, 7):
        send(st3.at[z], st3.at[z], dev(x, y, zm(d), c), "st3", "st3")
    sent("st1", st1.at[pl.ds(0, NX * NY - 1)])
    arrived("st3", st3.at[pl.ds(0, NZ - 1)])
    t_top, t_sum, w, s_top, s_sum = merged(st3, NZ)
    kl = w / t_sum - (t_top + jnp.log(t_sum)) + (s_top + jnp.log(s_sum))
    st4[dp] = jnp.broadcast_to(jnp.sum(kl, axis=1, keepdims=True), (8, 128))
    for d in (4, 5, 3, 2, 6, 7, 1):
        send(st4.at[dp], st4.at[dp], (lax.rem(dp + d, 8), v), "st4", "st4")
    kl_ref[...] = kl
    sent("st3", st3.at[pl.ds(0, NZ - 1)])
    arrived("st4", st4.at[pl.ds(0, 7)])
    total = st4[0]
    for k in range(1, 8):
        total += st4[k]
    loss_ref[...] = total * (1.0 / (TOK * 8))
    sent("st4", st4.at[pl.ds(0, 7)])
    assert set(s_bytes) == {"th"} and set(r_bytes) == {"th"}, (s_bytes, r_bytes)
    assert (len(s_index), len(r_index)) == (N_SEND, N_RECV), (len(s_index), len(r_index))


def hand_out(kl_in, loss_in, kl_ref, loss_ref):
    kl_ref[...] = kl_in[...]
    loss_ref[...] = loss_in[0:1, 0:1]


def shards(th, sh, tw, sw):
    hbm = pl.BlockSpec(memory_space=pl.ANY)
    vmem = pl.BlockSpec(memory_space=pltpu.VMEM)
    bf16 = jnp.bfloat16
    kl, loss = pl.pallas_call(
        body,
        out_shape=(
            pltpu.VMEM((1, TOK), F32),
            pltpu.VMEM((8, 128), F32),
        ),
        in_specs=[hbm] * 4,
        out_specs=(vmem, vmem),
        scratch_shapes=[
            pltpu.VMEM((TOK, TF), bf16),
            pltpu.VMEM((4 * TOK, NZ * TF), bf16),
            pltpu.VMEM((NZ, 4 * TOK, NX * SF), bf16),
            pltpu.VMEM((2 * VB, VB), bf16),
            pltpu.VMEM((NZ, NX * SF, CB), bf16),
            pltpu.VMEM((2, 2, SF, CB), bf16),
            pltpu.VMEM((4, 4 * TOK, CB), F32),
            pltpu.VMEM((4 * TOK, CB), F32),
            pltpu.VMEM((2, 4 * TOK, CB), F32),
            pltpu.VMEM((4 * TOK, CB), F32),
            pltpu.VMEM((NY, 8, 128), F32),
            pltpu.VMEM((NX * NY, 8, 128), F32),
            pltpu.VMEM((NZ, 8, 128), F32),
            pltpu.VMEM((8, 8, 128), F32),
            pltpu.SemaphoreType.DMA((N_SEND,)),
            pltpu.SemaphoreType.DMA((N_RECV,)),
            pltpu.SemaphoreType.DMA((5,)),
        ],
        compiler_params=pltpu.CompilerParams(
            collective_id=0, has_side_effects=True, vmem_limit_bytes=60 * 1024 * 1024
        ),
        name="kl_all",
    )(th, sh, tw, sw.reshape(4, SF, VB))
    vmem = pl.BlockSpec(memory_space=pltpu.VMEM)
    kl, loss = pl.pallas_call(
        hand_out,
        out_shape=(jax.ShapeDtypeStruct((1, TOK), F32), jax.ShapeDtypeStruct((1, 1), F32)),
        in_specs=[vmem] * 2,
        out_specs=(vmem, vmem),
        name="hand_out",
    )(*(pltpu.with_memory_space_constraint(a, pltpu.VMEM) for a in (kl, loss)))
    return (kl.reshape(TOK), loss.reshape(()))


def solution(mesh):
    in_specs = (P("dp", "vocab"),) * 4
    return jax.shard_map(
        shards, mesh=mesh, in_specs=in_specs, out_specs=(P("dp"), P()), check_vma=False
    )
```
